512 devices in a mesh: dp: 16 (over y, x), space: 32 (over z, core).
Axes of the slice: x: 4, y: 4, z: 16, core: 2. Of those that a mesh axis runs over, the one named last changes fastest.
Arguments:
- voxel_feats: bfloat16 [16, 4096, 256], P('dp', 'space'), may hold values from -6 to 6
- neighbours: int32 [16, 4096, 6], P('dp', 'space'), may hold values from 0 to 384
- wanted_rows: int32 [16, 32, 32, 8], P('dp', 'space'), may hold values from 0 to 127
- live_counts: int32 [16, 32], P('dp'), may hold values from 1 to 128, 3072 in all within a row
- block_choice: int32 [16, 64, 4], P('dp', 'space'), may hold values from 0 to 63, all different within a row
- conv_weight: bfloat16 [7, 256, 512], P(None, 'space'), may hold values from -0.125 to 0.125
- norm_gain: float32 [512], replicated, may hold values from 0.1 to 1.9
- input_weight: bfloat16 [512, 2304], P('space'), may hold values from -5 to 5
- output_weight: bfloat16 [768, 512], P('space'), may hold values from -0.21875 to 0.21875
- cotangent: bfloat16 [16, 4096, 512], P('dp', 'space'), may hold values from -6 to 6
Outputs:
- layer_output: bfloat16 [16, 4096, 512], P('dp', 'space')
- output_grad: float32 [768, 512], P('space')
The draws below stay inside these ranges and needn't reach their ends.
Inputs may be any that keep to these rules, and one draw needn't show every extreme that they name: `neighbours`: an entry below 128 names a row of the device's own shard, entry 128 + p * 8 + c names the row taken from peer p in slot c, and the largest value names an absent neighbour. `wanted_rows`: places within the peer's shard. `block_choice`: each row names distinct blocks.
All inputs are finite; a program needn't handle non-finite values.
Results may differ from the reference program's by a relative error of at most 0.025.
Values may be sent and summed in bfloat16 or wider, within the bound.
A program may use at most 64 MiB of HBM per device.

```python
import math
import jax
import jax.numpy as jnp
import numpy as np
from jax import lax

CIN = 256
WIDTH = 512
ATT = 768
HEADS = 12
HEAD_DIM = 64
TAPS = 7
TOK_DEV = 128
BLK = 64
CAP = 8
SEL = 4
SHAPES = 16
TOKENS = 4096
BLOCKS = 64
N_SPACE = 32


def draw_input_weight(key, part):
    initial = jnp.clip(jax.random.normal(key, (WIDTH, 3 * ATT), jnp.float32), -4.0, 4.0) * WIDTH ** (-0.5)
    aligned = -4.0 * initial[:, :ATT] + initial[:, ATT:2 * ATT]
    combined = jnp.concatenate([initial[:, :ATT], aligned, initial[:, 2 * ATT:]], axis=1)
    return combined.astype(jnp.bfloat16)


def draw_voxel_feats(key, part):
    shard_count = TOKENS // TOK_DEV
    shape_key = jax.random.fold_in(key, 17)
    region_key = jax.random.fold_in(key, 29)
    jitter_key = jax.random.fold_in(key, 41)
    shape_common = 0.65 * jax.random.normal(shape_key, (SHAPES, 1, 1, CIN), jnp.float32)
    region_part = 0.65 * jax.random.normal(region_key, (SHAPES, shard_count, 1, CIN), jnp.float32)
    jitter = 0.35 * jax.random.normal(jitter_key, (SHAPES, shard_count, TOK_DEV, CIN), jnp.float32)
    combined = (shape_common + region_part + jitter).reshape(SHAPES, TOKENS, CIN)
    return jnp.clip(combined, -6.0, 6.0).astype(jnp.bfloat16)


def place_ends(array, rng, least, high):
    shape = array.shape
    spot = [jax.random.randint(jax.random.fold_in(rng, axis), (), 0, shape[axis]) for axis in range(len(shape))]
    array = array.at[tuple(spot)].set(least)
    longest = shape.index(max(shape))
    spot[longest] = (spot[longest] + 1) % shape[longest]
    return array.at[tuple(spot)].set(high)


def level_of(key, shape, shards, smallest, largest):
    def one(position, parts):
        heights = jax.random.uniform(jax.random.fold_in(jax.random.fold_in(key, 6), position), (parts,), jnp.float32, smallest / len(shards), largest / len(shards))
        return jnp.repeat(jnp.exp(heights), shape[position] // parts).reshape((-1,) + (1,) * (len(shape) - position - 1))

    gain = one(*shards[0])
    for cut in shards[1:]:
        gain = gain * one(*cut)
    return gain


def distinct(rng, rows, number_of, top, lift):
    ranking = jax.random.permutation(jax.random.fold_in(rng, 1), number_of)
    pull = ranking
    for power in range(3):
        pull = pull * pull // number_of
    pull = pull * lift // number_of
    tickets = jax.random.randint(jax.random.fold_in(rng, 2), (rows, number_of), 0, 4096) + pull
    holders = jax.random.permutation(jax.random.fold_in(rng, 3), rows)[jnp.arange(number_of) % rows]
    tickets = jnp.where(jnp.arange(rows)[:, None] == holders[None, :], 1 << 14, tickets)
    priority = tickets * number_of + jnp.arange(number_of)
    return lax.top_k(priority.astype(jnp.int32), top)[1].astype(jnp.int32)


def profile(amount, total, bound, lean):
    loads = [(1 << 20) // math.isqrt(rank ** lean) + 1 for rank in range(2, amount + 1)]
    rest, given = total - bound - (amount - 1), [1] * (amount - 1)
    while rest > 0:
        free = [i for i in range(amount - 1) if given[i] < bound]
        whole, remaining = sum([loads[i] for i in free]), rest
        for i in free:
            addition = min(bound - given[i], max(1, remaining * loads[i] // whole), rest)
            given[i] = given[i] + addition
            rest = rest - addition
    return np.array([bound] + given)


def ragged_sizes(rng, count, total, reach, skew):
    if count == 2:
        one = jax.random.randint(rng, (), max(1, total - reach), min(reach, total - 1) + 1)
        return jnp.stack([one, total - one])
    sizes = jnp.asarray(profile(count, total, reach, skew), jnp.int32)
    pairs = (count - 1) // 2
    source_of, sink = sizes[1:1 + 2 * pairs:2], sizes[2:2 + 2 * pairs:2]
    slack = jnp.minimum(source_of - 1, reach - sink)
    passed = jax.random.randint(jax.random.fold_in(rng, 1), (pairs,), 0, 1 << 20) % (slack + 1)
    sizes = sizes.at[1:1 + 2 * pairs:2].set(source_of - passed).at[2:2 + 2 * pairs:2].set(sink + passed)
    return sizes[jax.random.permutation(jax.random.fold_in(rng, 2), count)]


def scatter_about(rng, extent, width, bound, split=(), held_as=jnp.bfloat16):
    loudness = level_of(rng, extent, split, -0.22, 0.18) if split else 1.0
    values = jax.random.normal(rng, extent, jnp.float32) * width * loudness
    return jnp.minimum(jnp.maximum(values, -bound), bound).astype(held_as)


def setup_inputs(seed: int = 0) -> dict:
    key_list = jax.random.split(jax.random.key(seed), 11)
    voxel_feats = draw_voxel_feats(jax.random.fold_in(key_list[10], 71), 0)
    neighbours = place_ends(jax.random.randint(key_list[1], (SHAPES, TOKENS, TAPS - 1), 0, TOK_DEV + N_SPACE * CAP + 1), jax.random.fold_in(key_list[1], 1), 0, TOK_DEV + N_SPACE * CAP).astype(jnp.int32)
    wanted_rows = place_ends(jax.random.randint(key_list[2], (SHAPES, N_SPACE, N_SPACE, CAP), 0, TOK_DEV), jax.random.fold_in(key_list[2], 1), 0, TOK_DEV - 1).astype(jnp.int32)
    live_counts = jax.vmap(lambda own: ragged_sizes(own, N_SPACE, TOKENS * 3 // 4, TOK_DEV, 2))(jax.random.split(key_list[3], SHAPES)).reshape((SHAPES, N_SPACE)).astype(jnp.int32)
    block_choice = distinct(key_list[4], SHAPES * BLOCKS, BLOCKS, SEL, 0).reshape((SHAPES, BLOCKS, SEL))
    conv_weight = scatter_about(key_list[5], (TAPS, CIN, WIDTH), (TAPS * CIN) ** -0.5, 0.125, ((1, 32),))
    norm_gain = jnp.clip(1.0 + 0.18 * jax.random.normal(key_list[6], (WIDTH,), jnp.float32), 0.1, 1.9)
    input_weight = draw_input_weight(jax.random.fold_in(key_list[10], 71), 0)
    output_weight = scatter_about(key_list[8], (ATT, WIDTH), ATT ** -0.5, 0.21875, ((0, 32),))
    cotangent = scatter_about(key_list[9], (SHAPES, TOKENS, WIDTH), 1.0, 6.0, ((0, 16), (1, 32)))
    return {"voxel_feats": voxel_feats, "neighbours": neighbours, "wanted_rows": wanted_rows, "live_counts": live_counts, "block_choice": block_choice, "conv_weight": conv_weight, "norm_gain": norm_gain, "input_weight": input_weight, "output_weight": output_weight, "cotangent": cotangent}


def attend(query, keys, values, key_live, short_keys, short_values):
    scale = HEAD_DIM ** (-0.5)
    query = query.astype(jnp.float32)
    near = jnp.einsum('bqhd,bkhd->bhqk', query, keys.astype(jnp.float32)) * scale
    near = jnp.where(key_live[:, None, None, :], near, -1e+30)
    far = jnp.einsum('bqhd,bshd->bhqs', query, short_keys.astype(jnp.float32)) * scale
    scores = jnp.concatenate([near, far], axis=-1)
    highest = lax.optimization_barrier(jnp.max(scores, axis=-1, keepdims=True))
    weights = jnp.exp(scores - highest)
    weights = (weights / lax.optimization_barrier(jnp.sum(weights, axis=-1, keepdims=True))).astype(jnp.bfloat16).astype(jnp.float32)
    mixed = jnp.einsum('bhqk,bkhd->bqhd', weights[..., :BLK], values.astype(jnp.float32))
    return mixed + jnp.einsum('bhqs,bshd->bqhd', weights[..., BLK:], short_values.astype(jnp.float32))

def one_shape(items, conv_weight, norm_gain, input_weight, output_weight):
    rows, index_map, lists, counts, chosen, upstream = items
    flat_weight = conv_weight.reshape(TAPS * CIN, WIDTH)
    positions = jnp.arange(TOKENS, dtype=jnp.int32)
    shard_of = positions // TOK_DEV
    place = positions % TOK_DEV
    owners = jnp.arange(N_SPACE, dtype=jnp.int32)[None, :, None] * TOK_DEV
    fetched = (owners + lists).reshape(N_SPACE, N_SPACE * CAP).astype(jnp.int32)
    absent = jnp.full((N_SPACE, 1), TOKENS, jnp.int32)
    lookup = jnp.concatenate([positions.reshape(N_SPACE, TOK_DEV), fetched, absent], axis=1)
    global_ids = jnp.take_along_axis(lookup, index_map.reshape(N_SPACE, TOK_DEV * (TAPS - 1)), axis=1)
    global_ids = global_ids.reshape(TOKENS, TAPS - 1)
    padded = jnp.concatenate([rows, jnp.zeros((1, CIN), jnp.bfloat16)], axis=0)
    taps = jnp.concatenate([rows[:, None, :], padded[global_ids]], axis=1).reshape(TOKENS, TAPS * CIN)
    live = place < counts[shard_of]
    live_f = live.astype(jnp.float32)
    hidden = jnp.dot(taps, flat_weight, preferred_element_type=jnp.float32) * live_f[:, None]
    power = lax.optimization_barrier(jnp.mean(hidden * hidden, axis=-1, keepdims=True))
    normed = (hidden * lax.rsqrt(power + 1e-06) * norm_gain).astype(jnp.bfloat16)
    projected = jnp.dot(normed, input_weight, preferred_element_type=jnp.float32).astype(jnp.bfloat16)
    query = projected[:, :ATT].reshape(BLOCKS, BLK, HEADS, HEAD_DIM)
    keys = projected[:, ATT:2 * ATT]
    values = projected[:, 2 * ATT:]
    block_live = live_f.reshape(BLOCKS, BLK)
    divisor = jnp.maximum(lax.optimization_barrier(jnp.sum(block_live, axis=1)), 1.0)[:, None]
    short_keys = (lax.optimization_barrier(jnp.sum(keys.astype(jnp.float32).reshape(BLOCKS, BLK, ATT) * block_live[:, :, None], axis=1)) / divisor).astype(jnp.bfloat16)
    short_values = (lax.optimization_barrier(jnp.sum(values.astype(jnp.float32).reshape(BLOCKS, BLK, ATT) * block_live[:, :, None], axis=1)) / divisor).astype(jnp.bfloat16)
    picked_keys = short_keys[chosen].reshape(BLOCKS, SEL, HEADS, HEAD_DIM)
    picked_values = short_values[chosen].reshape(BLOCKS, SEL, HEADS, HEAD_DIM)
    mixed = attend(query, keys.reshape(BLOCKS, BLK, HEADS, HEAD_DIM), values.reshape(BLOCKS, BLK, HEADS, HEAD_DIM), live.reshape(BLOCKS, BLK), picked_keys, picked_values)
    attended = (mixed.reshape(TOKENS, ATT) * live_f[:, None]).astype(jnp.bfloat16)
    layer = (hidden + jnp.dot(attended, output_weight, preferred_element_type=jnp.float32)).astype(jnp.bfloat16)
    grad_term = jnp.dot(attended.T, upstream, preferred_element_type=jnp.float32)
    return (layer, grad_term)

def reference(voxel_feats, neighbours, wanted_rows, live_counts, block_choice, conv_weight, norm_gain, input_weight, output_weight, cotangent):

    def runner(items):
        return one_shape(items, conv_weight, norm_gain, input_weight, output_weight)
    layers, terms = lax.map(runner, (voxel_feats, neighbours, wanted_rows, live_counts, block_choice, cotangent))
    factor = (SHAPES * TOKENS) ** (-0.5)
    return (layers, lax.optimization_barrier(jnp.sum(terms, axis=0)) * factor)
```

```python
import jax
import jax.numpy as jnp
from jax import lax
from jax.experimental import pallas as pl
from jax.experimental.pallas import tpu as pltpu
from jax.sharding import Mesh
from jax.sharding import PartitionSpec as P

MESH = pl.DeviceIdType.MESH
F32 = jnp.float32
BF16 = jnp.bfloat16
NZ = 16
CHUNKS = ((0, 2), (2, 4), (4, 5))


def iota(shape, dim):
    return lax.broadcasted_iota(jnp.int32, shape, dim)


def one_hot(flags):
    return jnp.where(flags, 1.0, 0.0).astype(BF16)


def ordering(parts):
    n = 256 * parts
    col = iota((1, n), 1)
    natural = ((col >> 3) & 15) * (16 * parts) + ((col >> 7) & 1) * (8 * parts) + (col >> 8) * 8 + (col & 7)
    return one_hot(iota((n, n), 0) == natural)


def dot(a, b):
    return jnp.dot(a, b, preferred_element_type=F32)


def dot_t(a, b):
    return lax.dot_general(a, b, (((1,), (1,)), ((), ())), preferred_element_type=F32)


def drain(ref, sem):
    pltpu.make_async_copy(ref, ref, sem).wait()


def kernel(
    feats, near_map, wanted, counts, choice, conv_h, gain, inw_h, outw_h, cot_h,
    layer, grad,
    asked, asks, table, answers, own_feats, taps_hot, taps, staged, held,
    hidden, qkv, tall, shorts, picked, split_q, scores, cot, att, terms, across, summed, along, final,
    order_in, order_out,
    local_sem, send_sem, recv_sem,
):
    y, x, z, c = (lax.axis_index(n) for n in ("y", "x", "z", "c"))
    other = 1 - c
    me = z * 2 + c
    plane = y * 4 + x
    a = (1 - c) * x + c * y
    b = (1 - c) * y + c * x
    piece = b * 4 + a

    def z_of(i):
        return lax.rem(z + 8 + (1 - 2 * lax.rem(i, 2)) * ((i + 1) // 2), NZ)

    def a_peer(d):
        t = lax.rem(a + d, 4)
        return t, {"x": (1 - c) * t + c * x, "y": (1 - c) * y + c * t}

    def b_peer(d):
        t = lax.rem(b + d, 4)
        return {"x": (1 - c) * x + c * t, "y": (1 - c) * t + c * y}

    def plane_peer(k):
        t = lax.rem(plane + k, 16)
        return {"y": t // 4, "x": lax.rem(t, 4)}

    def send(src, dst, s, r, where):
        pltpu.make_async_remote_copy(
            src_ref=src, dst_ref=dst, send_sem=send_sem.at[s], recv_sem=recv_sem.at[r],
            device_id=where, device_id_type=MESH,
        ).start()

    def fetch(src, dst, k):
        copy = pltpu.make_async_copy(src, dst, local_sem.at[k])
        copy.start()
        return copy

    lanes = pl.ds(pl.multiple_of(a * 128, 128), 128)
    copies = [
        fetch(cot_h.at[0], cot.at[c], 0),
        fetch(conv_h.at[2 * b, :, lanes], staged.at[0], 1),
        fetch(inw_h.at[pl.ds(0, 8), pl.ds(pl.multiple_of(piece * 128, 128), 128)], staged.at[2], 3),
        fetch(inw_h.at[pl.ds(8, 8), pl.ds(pl.multiple_of(piece * 128, 128), 128)], staged.at[3], 4),
        fetch(outw_h.at[pl.ds(pl.multiple_of(lax.rem(b, 3) * 8, 8), 8), lanes], staged.at[4], 5),
    ]

    @pl.when(b < 3)
    def _():
        fetch(conv_h.at[2 * b + 1, :, lanes], staged.at[1], 2)

    @pl.when(b == 3)
    def _():
        fetch(
            inw_h.at[pl.ds(pl.multiple_of(lax.rem(a, 2) * 8, 8), 8), pl.ds(pl.multiple_of((16 + a // 2) * 128, 128), 128)],
            staged.at[1], 2,
        )

    barrier = pltpu.get_barrier_semaphore()

    def hail(where):
        pl.semaphore_signal(barrier, inc=1, device_id=where, device_id_type=MESH)

    def hail_z(i, _):
        hail({"z": z_of(i), "c": 0})
        hail({"z": z_of(i), "c": 1})
        return 0

    lax.fori_loop(0, NZ - 1, hail_z, 0)
    lax.fori_loop(1, 16, lambda k, _: (hail(plane_peer(k)), 0)[1], 0)
    hail({"c": other})

    asks[...] = jnp.zeros_like(asks)
    for p in range(32):
        asks[p, :, 0:8] = wanted[0, 0, p : p + 1, :]
    for copy in copies:
        copy.wait()
    drain(staged.at[1], local_sem.at[2])
    held[piece, :, c, z] = staged[...]
    asked[me] = asks[me]
    ordered = dot(feats[0], ordering(1)).astype(BF16)
    own_feats[...] = ordered
    table[0:16] = ordered.reshape(16, 8, 256)
    for k in range(6):
        taps_hot[128 * k : 128 * (k + 1), :] = one_hot(near_map[0, :, k : k + 1] == iota((128, 384), 1))
    pl.semaphore_wait(barrier, 46)

    def ask(i, _):
        t = z_of(i)
        for core in range(2):
            send(asks.at[t * 2 + core], asked.at[me], 0, 0, {"z": t, "c": core})
        return 0

    lax.fori_loop(0, NZ - 1, ask, 0)
    send(asks.at[z * 2 + other], asked.at[me], 0, 0, {"c": other})
    for n, (lo, hi) in enumerate(CHUNKS):

        def spread(i, _, n=n, lo=lo, hi=hi):
            send(staged.at[lo:hi], held.at[piece, lo:hi, c, z], 1 + n, 1 + n, {"z": z_of(i)})
            return 0

        lax.fori_loop(0, NZ - 1, spread, 0)
    send(cot.at[c], cot.at[c], 4, 4, {"c": other})

    order_in[...] = ordering(2)
    order_out[...] = ordering(3)

    drain(asked.at[0:31], recv_sem.at[0])
    lists = asked[:, 0, :].astype(F32).astype(BF16)
    spread_out = dot(one_hot((iota((256, 32), 0) >> 3) == iota((256, 32), 1)), lists)
    lane = iota((256, 128), 1)
    row = jnp.sum(jnp.where(lane == (iota((256, 128), 0) & 7), spread_out, 0.0), axis=1, keepdims=True)
    picked_rows = dot(one_hot(row == lane.astype(F32)), own_feats[...]).astype(BF16)
    answers[...] = picked_rows.reshape(32, 8, 256)
    table[16 + me] = answers[me]

    def answer(i, _):
        t = z_of(i)
        for core in range(2):
            send(answers.at[t * 2 + core], table.at[16 + me], 5, 5, {"z": t, "c": core})
        return 0

    lax.fori_loop(0, NZ - 1, answer, 0)
    send(answers.at[z * 2 + other], table.at[16 + me], 5, 5, {"c": other})

    for n, (lo, hi) in enumerate(CHUNKS):
        drain(held.at[0, lo:hi, 0, 0:15], recv_sem.at[1 + n])
        for d in range(1, 4):
            part = held.at[piece, lo:hi, c]
            send(part, part, 6 + n, 6 + n, a_peer(d)[1])
    for n, (lo, hi) in enumerate(CHUNKS):
        drain(held.at[0:3, lo:hi, 0], recv_sem.at[6 + n])
        part = held.at[pl.ds(b * 4, 4), lo:hi, c]
        for d in range(1, 4):
            send(part, part, 9 + n, 9 + 3 * n + d - 1, b_peer(d))
        send(part, part, 12 + n, 18 + n, {"c": other})

    def cross(n):
        lo, hi = CHUNKS[n]
        for d in range(1, 4):
            part = held.at[pl.ds(lax.rem(b + 4 - d, 4) * 4, 4), lo:hi, c]
            drain(part, recv_sem.at[9 + 3 * n + d - 1])
            send(part, part, 12 + n, 18 + n, {"c": other})

    def crossed(n):
        lo, hi = CHUNKS[n]
        drain(held.at[:, lo:hi, 0], recv_sem.at[18 + n])

    drain(table.at[0:31], recv_sem.at[5])
    for k in range(3):
        got = dot(taps_hot[256 * k : 256 * (k + 1), :], table[...].reshape(384, 256))
        taps[2 * k : 2 * k + 2] = got.astype(BF16).reshape(2, 128, 256)
    cross(0)
    crossed(0)

    def unit(p, u):
        return held[p, u].reshape(256, 128)

    count = counts[0, me]
    alive = jnp.where(iota((128, 128), 0) < count, 1.0, 0.0)
    alive_wide = jnp.concatenate([alive, alive], axis=1)
    for t in range(0, 4, 2):
        total = jnp.zeros((128, 256), F32)
        for k in range(7):
            p, u = (k // 2) * 4 + t, k % 2
            tap = own_feats[...] if k == 0 else taps[k - 1]
            total = total + dot(tap, jnp.concatenate([unit(p, u), unit(p + 1, u)], axis=1))
        hidden[:, 128 * t : 128 * (t + 2)] = total * alive_wide
    h = hidden[...]
    power = jnp.mean(h * h, axis=-1, keepdims=True)
    normed = (h * lax.rsqrt(power + 1e-06) * gain[...]).astype(BF16)
    normed = dot(normed, order_in[...]).astype(BF16)
    cross(1)
    crossed(1)

    def project(j):
        upper, lower = [], []
        for t in (j, j + 1):
            if t < 16:
                upper.append(unit(t, 2))
                lower.append(unit(t, 3))
            else:
                upper.append(unit(12 + 2 * (t - 16), 1))
                lower.append(unit(13 + 2 * (t - 16), 1))
        got = dot(normed[:, :256], jnp.concatenate(upper, axis=1))
        got = got + dot(normed[:, 256:], jnp.concatenate(lower, axis=1))
        qkv[:, 128 * j : 128 * (j + 2)] = got.astype(BF16)

    for j in range(6, 18, 2):
        project(j)

    token = iota((8, 128), 1)
    block_mask = one_hot(((token >> 6) == iota((8, 128), 0)) & (token < count))
    sums = dot(block_mask, qkv[:, 768:])
    number = jnp.clip(count - 64 * iota((8, 1), 0), 0, 64)
    means = sums / jnp.maximum(number, 1).astype(F32)
    for j in range(12):
        tall[2 * j : 2 * j + 2, :] = means[0:2, 128 * j : 128 * (j + 1)]
    shorts[c, z] = tall[...].astype(BF16).reshape(3, 8, 128)

    def tell(i, _):
        send(shorts.at[c, z], shorts.at[c, z], 15, 21, {"z": z_of(i)})
        return 0

    lax.fori_loop(0, NZ - 1, tell, 0)

    for j in range(0, 6, 2):
        project(j)
    half = iota((128, 128), 1) < 64
    row256 = iota((256, 128), 0) & 127
    col256 = iota((256, 128), 1)
    near_ok = ((row256 >> 6) == (col256 >> 6)) & (col256 < count)
    for j in range(6):
        q = qkv[:, 128 * j : 128 * (j + 1)] * jnp.asarray(0.125, BF16)
        none = jnp.zeros_like(q)
        q = jnp.concatenate([jnp.where(half, q, none), jnp.where(half, none, q)], axis=0)
        split_q[j] = q
        scores[j] = jnp.where(near_ok, dot_t(q, qkv[:, 768 + 128 * j : 768 + 128 * (j + 1)]), -1e30)
    m96 = iota((96, 1), 0)
    target = jnp.zeros((96, 1), jnp.int32)
    for e in range(8):
        block = choice[0, e // 4, e % 4]
        shard = block // 2
        start = (lax.rem(shard, 2) * 16 + shard // 2) * 24 + lax.rem(block, 2)
        target = jnp.where((m96 & 7) == e, start, target)
    target = target + 2 * (m96 >> 3)
    chosen_hot = one_hot(target == iota((96, 768), 1))
    cross(2)

    drain(shorts.at[0, 0:15], recv_sem.at[21])
    send(shorts.at[c], shorts.at[c], 16, 22, {"c": other})
    drain(shorts.at[0], recv_sem.at[22])
    picked[...] = dot(chosen_hot, shorts[...].reshape(768, 128))
    far_ok = ((iota((256, 8), 0) & 127) >> 6) == (iota((256, 8), 1) >> 2)
    for j in range(6):
        near = scores[j]
        far = dot_t(split_q[j], picked[8 * j : 8 * j + 8, :].astype(BF16))
        far = jnp.where(far_ok, far, -1e30)
        top = jnp.maximum(jnp.max(near, axis=1, keepdims=True), jnp.max(far, axis=1, keepdims=True))
        near, far = jnp.exp(near - top), jnp.exp(far - top)
        scale = 1.0 / (jnp.sum(near, axis=1, keepdims=True) + jnp.sum(far, axis=1, keepdims=True))
        near, far = (near * scale).astype(BF16), (far * scale).astype(BF16)
        mixed = dot(near, qkv[:, 1536 + 128 * j : 1536 + 128 * (j + 1)])
        mixed = mixed + dot(far, picked[48 + 8 * j : 56 + 8 * j, :].astype(BF16))
        mixed = jnp.where(half, mixed[:128], mixed[128:]) * alive
        att[c, :, 128 * j : 128 * (j + 1)] = mixed.astype(BF16)

    send(att.at[c], att.at[c], 17, 23, {"c": other})
    drain(cot.at[0], recv_sem.at[4])
    drain(att.at[0], recv_sem.at[23])
    both = att[...].reshape(256, 768)
    for t in range(0, 4, 2):
        g = lax.dot_general(
            both, cot[:, :, 128 * t : 128 * (t + 2)].reshape(256, 256), (((0,), (0,)), ((), ())), preferred_element_type=F32
        )
        for s in range(2):
            terms[t + s] = g[:, 128 * s : 128 * (s + 1)].astype(BF16).reshape(NZ, 2, 3, 8, 128)
    for d in range(1, 4):
        t, where = a_peer(d)
        send(terms.at[t, :, c], across.at[d - 1], 18, 24, where)

    crossed(2)
    attended = dot(att[c], order_out[...]).astype(BF16)
    for t in range(0, 4, 2):
        total = hidden[:, 128 * t : 128 * (t + 2)]
        for i in range(3):
            w = jnp.concatenate([unit(4 * i + t, 4), unit(4 * i + t + 1, 4)], axis=1)
            total = total + dot(attended[:, 256 * i : 256 * (i + 1)], w)
        layer[0, :, 128 * t : 128 * (t + 2)] = total.astype(BF16)

    drain(across, recv_sem.at[24])
    total = terms[a, :, c].astype(F32)
    for d in range(3):
        total = total + across[d].astype(F32)
    summed[...] = total.astype(BF16)
    along[z] = summed[z]

    def reduce_z(i, _):
        t = z_of(i)
        send(summed.at[t], along.at[z], 19, 25, {"z": t})
        return 0

    lax.fori_loop(0, NZ - 1, reduce_z, 0)
    drain(along.at[0:15], recv_sem.at[25])
    total = along[0].astype(F32)
    for k in range(1, NZ):
        total = total + along[k].astype(F32)
    final[piece] = total.astype(BF16)

    def show(k, _):
        send(final.at[piece], final.at[piece], 20, 26, plane_peer(k))
        return 0

    lax.fori_loop(1, 16, show, 0)
    drain(final.at[0:15], recv_sem.at[26])
    factor = (16 * 4096) ** -0.5
    for t in range(4):
        total = final[t].astype(F32)
        for k in range(1, 4):
            total = total + final[4 * k + t].astype(F32)
        grad[:, 128 * t : 128 * (t + 1)] = total.reshape(24, 128) * factor

    drain(asked.at[0:31], send_sem.at[0])
    for n, (lo, hi) in enumerate(CHUNKS):
        drain(held.at[0, lo:hi, 0, 0:15], send_sem.at[1 + n])
        drain(held.at[0:3, lo:hi, 0], send_sem.at[6 + n])
        drain(held.at[0:12, lo:hi, 0], send_sem.at[9 + n])
        drain(held.at[:, lo:hi, 0], send_sem.at[12 + n])
    drain(cot.at[0], send_sem.at[4])
    drain(table.at[0:31], send_sem.at[5])
    drain(shorts.at[0, 0:15], send_sem.at[15])
    drain(shorts.at[0], send_sem.at[16])
    drain(att.at[0], send_sem.at[17])
    drain(across, send_sem.at[18])
    drain(along.at[0:15], send_sem.at[19])
    drain(final.at[0:15], send_sem.at[20])


def shards(feats, near_map, wanted, counts, choice, conv, gain, inw, outw, cot):
    vmem = pl.BlockSpec(memory_space=pltpu.VMEM)
    smem = pl.BlockSpec(memory_space=pltpu.SMEM)
    anywhere = pl.BlockSpec(memory_space=pl.ANY)
    v = pltpu.VMEM
    return pl.pallas_call(
        kernel,
        name="layer",
        out_shape=(jax.ShapeDtypeStruct((1, 128, 512), BF16), jax.ShapeDtypeStruct((24, 512), F32)),
        in_specs=[vmem, vmem, vmem, smem, smem, anywhere, vmem, anywhere, anywhere, anywhere],
        out_specs=(vmem, vmem),
        scratch_shapes=[
            v((32, 1, 128), jnp.int32),
            v((32, 1, 128), jnp.int32),
            v((48, 8, 256), BF16),
            v((32, 8, 256), BF16),
            v((128, 256), BF16),
            v((768, 384), BF16),
            v((6, 128, 256), BF16),
            v((5, 8, 128), BF16),
            v((16, 5, 2, NZ, 8, 128), BF16),
            v((128, 512), F32),
            v((128, 2304), BF16),
            v((24, 128), F32),
            v((2, NZ, 3, 8, 128), BF16),
            v((96, 128), F32),
            v((6, 256, 128), BF16),
            v((6, 256, 128), F32),
            v((2, 128, 512), BF16),
            v((2, 128, 768), BF16),
            v((4, NZ, 2, 3, 8, 128), BF16),
            v((3, NZ, 3, 8, 128), BF16),
            v((NZ, 3, 8, 128), BF16),
            v((NZ, 3, 8, 128), BF16),
            v((16, 3, 8, 128), BF16),
            v((512, 512), BF16),
            v((768, 768), BF16),
            pltpu.SemaphoreType.DMA((6,)),
            pltpu.SemaphoreType.DMA((21,)),
            pltpu.SemaphoreType.DMA((27,)),
        ],
        compiler_params=pltpu.CompilerParams(
            collective_id=0, has_side_effects=True, vmem_limit_bytes=48 * 1024 * 1024
        ),
    )(feats, near_map, wanted, counts, choice, conv, gain.reshape(1, -1), inw, outw, cot)


def solution(mesh):
    space = ("z", "c")
    dp = ("y", "x")
    torus = Mesh(mesh.devices.reshape(4, 4, 16, 2), dp + space)
    return jax.shard_map(
        shards,
        mesh=torus,
        in_specs=(
            P(dp, space, None),
            P(dp, space, None),
            P(dp, space, None, None),
            P(dp, None),
            P(dp, space, None),
            P(None, space, None),
            P(),
            P(space, None),
            P(space, None),
            P(dp, space, None),
        ),
        out_specs=(P(dp, space, None), P(space, None)),
        check_vma=False,
    )
```

```python
import jax
import jax.numpy as jnp
from jax import lax
from jax.experimental import pallas as pl
from jax.experimental.pallas import tpu as pltpu
from jax.sharding import Mesh
from jax.sharding import PartitionSpec as P

MESH = pl.DeviceIdType.MESH
F32 = jnp.float32
BF16 = jnp.bfloat16
NZ = 16
VMEM = 48 * 1024 * 1024
CHUNKS = ((0, 2, 0, 8), (0, 2, 8, 16), (2, 4, 0, 8), (2, 4, 8, 16), (4, 5, 0, 16))


def iota(shape, dim):
    return lax.broadcasted_iota(jnp.int32, shape, dim)


def one_hot(flags):
    return jnp.where(flags, 1.0, 0.0).astype(BF16)


def ordering(parts, z):
    n = 256 * parts
    col = iota((1, n), 1)
    slot = (col >> 3) & 15
    chip = (z + NZ + jnp.where((slot & 1) == 1, (slot + 1) >> 1, -(slot >> 1))) & 15
    natural = chip * (16 * parts) + ((col >> 7) & 1) * (8 * parts) + (col >> 8) * 8 + (col & 7)
    return one_hot(iota((n, n), 0) == natural)


def dot(a, b):
    return jnp.dot(a, b, preferred_element_type=F32)


def dot_t(a, b):
    return lax.dot_general(a, b, (((1,), (1,)), ((), ())), preferred_element_type=F32)


def drain(ref, sem):
    pltpu.make_async_copy(ref, ref, sem).wait()


def kernel(
    feats_h, near_h, wanted_h, counts_h, choice_h, conv_h, gain_h, inw_h, outw_h, cot_h,
    layer, grad,
    feats, near_map, wanted, counts, choice, gain, turned,
    asked, asks, table, answers, own_feats, taps_hot, taps, staged, held,
    hidden, qkv, tall, shorts, picked, split_q, scores, cot, att, terms, across, summed, along, final,
    order_taps, order_in, order_out,
    local_sem, send_sem, recv_sem,
):
    y, x, z, c = (lax.axis_index(n) for n in ("y", "x", "z", "c"))
    other = 1 - c
    me = z * 2 + c
    plane = y * 4 + x
    a = (1 - c) * x + c * y
    b = (1 - c) * y + c * x
    piece = b * 4 + a

    def z_of(slot):
        return lax.rem(z + NZ - (2 * lax.rem(slot, 2) - 1) * ((slot + 1) // 2), NZ)

    def a_peer(d):
        t = lax.rem(a + d, 4)
        return t, {"x": (1 - c) * t + c * x, "y": (1 - c) * y + c * t}

    def b_peer(d):
        t = lax.rem(b + d, 4)
        return t, {"x": (1 - c) * x + c * t, "y": (1 - c) * t + c * y}

    def plane_peer(k):
        t = lax.rem(plane + k, 16)
        return {"y": t // 4, "x": lax.rem(t, 4)}

    def send(src, dst, s, r, where):
        pltpu.make_async_remote_copy(
            src_ref=src, dst_ref=dst, send_sem=send_sem.at[s], recv_sem=recv_sem.at[r],
            device_id=where, device_id_type=MESH,
        ).start()

    def fetch(src, dst, k):
        copy = pltpu.make_async_copy(src, dst, local_sem.at[k])
        copy.start()
        return copy

    lanes = pl.ds(pl.multiple_of(a * 128, 128), 128)
    first = [
        fetch(wanted_h, wanted, 6),
        fetch(near_h, near_map, 7),
        fetch(feats_h.at[0], feats, 8),
    ]
    later = [
        fetch(counts_h, counts, 9),
        fetch(choice_h, choice, 10),
        fetch(gain_h, gain, 11),
    ]
    copies = [
        fetch(cot_h.at[0], cot.at[c], 0),
        fetch(conv_h.at[2 * b, :, lanes], staged.at[0], 1),
        fetch(inw_h.at[pl.ds(0, 8), pl.ds(pl.multiple_of(piece * 128, 128), 128)], staged.at[2], 3),
        fetch(inw_h.at[pl.ds(8, 8), pl.ds(pl.multiple_of(piece * 128, 128), 128)], staged.at[3], 4),
        fetch(outw_h.at[pl.ds(pl.multiple_of(lax.rem(b, 3) * 8, 8), 8), lanes], staged.at[4], 5),
    ]

    @pl.when(b < 3)
    def _():
        fetch(conv_h.at[2 * b + 1, :, lanes], staged.at[1], 2)

    @pl.when(b == 3)
    def _():
        fetch(
            inw_h.at[pl.ds(pl.multiple_of(lax.rem(a, 2) * 8, 8), 8), pl.ds(pl.multiple_of((16 + a // 2) * 128, 128), 128)],
            staged.at[1], 2,
        )

    barrier = pltpu.get_barrier_semaphore()

    def hail(where):
        pl.semaphore_signal(barrier, inc=1, device_id=where, device_id_type=MESH)

    def hail_z(i, _):
        hail({"z": z_of(i), "c": 0})
        hail({"z": z_of(i), "c": 1})
        return 0

    lax.fori_loop(1, NZ, hail_z, 0)
    lax.fori_loop(1, 16, lambda k, _: (hail(plane_peer(k)), 0)[1], 0)
    hail({"c": other})

    turned[...] = jnp.zeros_like(turned)
    for copy in first:
        copy.wait()
    turned[0, 0:8, 0:32] = wanted[0, 0].astype(F32)
    for k in range(6):
        turned[1, k : k + 1, :] = near_map[k].astype(F32)
    lists = turned[0].T.astype(jnp.int32)
    for p in range(32):
        asks[p] = lists[p : p + 1, :]
    asked[me] = asks[me]
    rows = turned[1].T
    for k in range(6):
        taps_hot[128 * k : 128 * (k + 1), :] = one_hot(rows[:, k : k + 1].astype(jnp.int32) == iota((128, 384), 1))
    order_taps[...] = ordering(1, z)
    ordered = dot(feats[...], order_taps[...]).astype(BF16)
    own_feats[...] = ordered
    table[0:16] = ordered.reshape(16, 8, 256)
    for copy in copies:
        copy.wait()
    drain(staged.at[1], local_sem.at[2])
    held[piece, :, c, 0] = staged[...]
    with jax.named_scope("w_barrier"):
        pl.semaphore_wait(barrier, 46)

    def far_first(body):
        lax.fori_loop(1, NZ, lambda i, _: (body(NZ - i), 0)[1], 0)

    def ask(slot):
        t = z_of(slot)
        for core in range(2):
            send(asks.at[t * 2 + core], asked.at[me], 0, 0, {"z": t, "c": core})

    def spread(n):
        lo, hi, s0, s1 = CHUNKS[n]

        def one(slot, _):
            send(staged.at[lo:hi], held.at[piece, lo:hi, c, slot], 5 + n, 7 + n, {"z": z_of(slot)})
            return 0

        lax.fori_loop(max(s0, 1), s1, one, 0)

    far_first(ask)
    send(asks.at[z * 2 + other], asked.at[me], 0, 0, {"c": other})
    for n in range(4):
        spread(n)
    send(cot.at[c], cot.at[c], 1, 1, {"c": other})
    for copy in later:
        copy.wait()
    order_in[...] = ordering(2, z)
    order_out[...] = ordering(3, z)

    def part(n, p, count, from_slot=None, to_slot=None):
        lo, hi, s0, s1 = CHUNKS[n]
        return held.at[pl.ds(p, count), lo:hi, c, s0 if from_slot is None else from_slot : s1 if to_slot is None else to_slot]

    def cross(n, p, count, *slots):
        some = part(n, p, count, *slots)
        send(some, some, 20 + n, 32 + n, {"c": other})

    def along_a(n):
        lo, hi, s0, s1 = CHUNKS[n]
        with jax.named_scope(f"w_z{n}"):
            drain(held.at[0, lo:hi, 0, max(s0, 1) : s1], recv_sem.at[7 + n])
        for d in (2, 1, 3):
            send(part(n, piece, 1), part(n, piece, 1), 10 + n, 12 + n, a_peer(d)[1])

    def along_b(n):
        lo, hi, s0, s1 = CHUNKS[n]
        with jax.named_scope(f"w_a{n}"):
            drain(held.at[0:3, lo:hi, 0, s0:s1], recv_sem.at[12 + n])
        for k, d in enumerate((1, 3)):
            send(part(n, b * 4, 4), part(n, b * 4, 4), 15 + n, 17 + 5 * k + n, b_peer(d)[1])
        cross(n, b * 4, 4)

    def relay(n):
        lo, hi, s0, s1 = CHUNKS[n]
        middle = (s0 + s1) // 2
        for k, d, low, high in ((0, 1, s0, middle), (1, 3, middle, s1)):
            source = lax.rem(b + 4 - d, 4) * 4
            with jax.named_scope(f"w_b{n}"):
                drain(part(n, source, 4), recv_sem.at[17 + 5 * k + n])
            send(part(n, source, 4, low, high), part(n, source, 4, low, high), 15 + n, 27 + n, b_peer(d)[1])
            cross(n, source, 4)

    def last(n):
        source = lax.rem(b + 2, 4) * 4
        with jax.named_scope(f"w_f{n}"):
            drain(part(n, source, 4), recv_sem.at[27 + n])
        cross(n, source, 4)

    def crossed(n):
        lo, hi, s0, s1 = CHUNKS[n]
        with jax.named_scope(f"w_c{n}"):
            drain(held.at[:, lo:hi, 0, s0:s1], recv_sem.at[32 + n])

    along_a(0)

    with jax.named_scope("w_ask"):
        drain(asked.at[0:31], recv_sem.at[0])
    lists = asked[:, 0, :].astype(F32).astype(BF16)
    spread_out = dot(one_hot((iota((256, 32), 0) >> 3) == iota((256, 32), 1)), lists)
    lane = iota((256, 128), 1)
    row = jnp.sum(jnp.where(lane == (iota((256, 128), 0) & 7), spread_out, 0.0), axis=1, keepdims=True)
    picked_rows = dot(one_hot(row == lane.astype(F32)), feats[...]).astype(BF16)
    answers[...] = picked_rows.reshape(32, 8, 256)
    table[16 + me] = answers[me]

    def answer(slot):
        t = z_of(slot)
        for core in range(2):
            send(answers.at[t * 2 + core], table.at[16 + me], 2, 2, {"z": t, "c": core})

    far_first(answer)
    send(answers.at[z * 2 + other], table.at[16 + me], 2, 2, {"c": other})
    spread(4)

    along_b(0)
    along_a(1)
    along_a(2)
    relay(0)
    along_b(1)
    along_a(3)
    along_b(2)
    relay(1)
    last(0)
    along_b(3)
    relay(2)
    last(1)
    with jax.named_scope("w_rows"):
        drain(table.at[0:31], recv_sem.at[2])
    fetched = table[16:48].reshape(256, 256)
    table[16:48] = dot(fetched, order_taps[...]).astype(BF16).reshape(32, 8, 256)
    for k in range(3):
        got = dot(taps_hot[256 * k : 256 * (k + 1), :], table[...].reshape(384, 256))
        taps[2 * k : 2 * k + 2] = got.astype(BF16).reshape(2, 128, 256)
    relay(3)
    last(2)
    crossed(0)
    crossed(1)

    def unit(p, u):
        return held[p, u].reshape(256, 128)

    count = counts[0, me]
    alive = jnp.where(iota((128, 128), 0) < count, 1.0, 0.0)
    alive_wide = jnp.concatenate([alive, alive], axis=1)
    for t in range(0, 4, 2):
        total = jnp.zeros((128, 256), F32)
        for k in range(7):
            p, u = (k // 2) * 4 + t, k % 2
            tap = own_feats[...] if k == 0 else taps[k - 1]
            total = total + dot(tap, jnp.concatenate([unit(p, u), unit(p + 1, u)], axis=1))
        hidden[:, 128 * t : 128 * (t + 2)] = total * alive_wide
    h = hidden[...]
    power = jnp.mean(h * h, axis=-1, keepdims=True)
    normed = (h * lax.rsqrt(power + 1e-06) * gain[...]).astype(BF16)
    normed = dot(normed, order_in[...]).astype(BF16)
    last(3)
    crossed(2)
    crossed(3)

    def project(j):
        upper, lower = [], []
        for t in (j, j + 1):
            if t < 16:
                upper.append(unit(t, 2))
                lower.append(unit(t, 3))
            else:
                upper.append(unit(12 + 2 * (t - 16), 1))
                lower.append(unit(13 + 2 * (t - 16), 1))
        got = dot(normed[:, :256], jnp.concatenate(upper, axis=1))
        got = got + dot(normed[:, 256:], jnp.concatenate(lower, axis=1))
        qkv[:, 128 * j : 128 * (j + 2)] = got.astype(BF16)

    for j in range(6, 18, 2):
        project(j)

    token = iota((8, 128), 1)
    block_mask = one_hot(((token >> 6) == iota((8, 128), 0)) & (token < count))
    sums = dot(block_mask, qkv[:, 768:])
    number = jnp.clip(count - 64 * iota((8, 1), 0), 0, 64)
    means = sums / jnp.maximum(number, 1).astype(F32)
    for j in range(12):
        tall[2 * j : 2 * j + 2, :] = means[0:2, 128 * j : 128 * (j + 1)]
    shorts[c, z] = tall[...].astype(BF16).reshape(3, 8, 128)

    far_first(lambda slot: send(shorts.at[c, z], shorts.at[c, z], 3, 3, {"z": z_of(slot)}))
    along_a(4)

    for j in range(0, 6, 2):
        project(j)
    half = iota((128, 128), 1) < 64
    row256 = iota((256, 128), 0) & 127
    col256 = iota((256, 128), 1)
    near_ok = ((row256 >> 6) == (col256 >> 6)) & (col256 < count)
    for j in range(6):
        q = qkv[:, 128 * j : 128 * (j + 1)] * jnp.asarray(0.125, BF16)
        none = jnp.zeros_like(q)
        q = jnp.concatenate([jnp.where(half, q, none), jnp.where(half, none, q)], axis=0)
        split_q[j] = q
        scores[j] = jnp.where(near_ok, dot_t(q, qkv[:, 768 + 128 * j : 768 + 128 * (j + 1)]), -1e30)
    m96 = iota((96, 1), 0)
    target = jnp.zeros((96, 1), jnp.int32)
    for e in range(8):
        block = choice[0, e // 4, e % 4]
        shard = block // 2
        start = (lax.rem(shard, 2) * 16 + shard // 2) * 24 + lax.rem(block, 2)
        target = jnp.where((m96 & 7) == e, start, target)
    target = target + 2 * (m96 >> 3)
    chosen_hot = one_hot(target == iota((96, 768), 1))
    along_b(4)
    relay(4)
    last(4)

    with jax.named_scope("w_short"):
        drain(shorts.at[0, 0:15], recv_sem.at[3])
    send(shorts.at[c], shorts.at[c], 4, 4, {"c": other})
    with jax.named_scope("w_shortc"):
        drain(shorts.at[0], recv_sem.at[4])
    picked[...] = dot(chosen_hot, shorts[...].reshape(768, 128))
    far_ok = ((iota((256, 8), 0) & 127) >> 6) == (iota((256, 8), 1) >> 2)
    for j in range(6):
        near = scores[j]
        far = dot_t(split_q[j], picked[8 * j : 8 * j + 8, :].astype(BF16))
        far = jnp.where(far_ok, far, -1e30)
        top = jnp.maximum(jnp.max(near, axis=1, keepdims=True), jnp.max(far, axis=1, keepdims=True))
        near, far = jnp.exp(near - top), jnp.exp(far - top)
        scale = 1.0 / (jnp.sum(near, axis=1, keepdims=True) + jnp.sum(far, axis=1, keepdims=True))
        near, far = (near * scale).astype(BF16), (far * scale).astype(BF16)
        mixed = dot(near, qkv[:, 1536 + 128 * j : 1536 + 128 * (j + 1)])
        mixed = mixed + dot(far, picked[48 + 8 * j : 56 + 8 * j, :].astype(BF16))
        mixed = jnp.where(half, mixed[:128], mixed[128:]) * alive
        att[c, :, 128 * j : 128 * (j + 1)] = mixed.astype(BF16)
        if j % 3 == 2:
            part_of = att.at[c, :, 128 * (j - 2) : 128 * (j + 1)]
            send(part_of, part_of, 25 + j // 3, 5 + j // 3, {"c": other})

    drain(cot.at[0], recv_sem.at[1])
    for g in range(2):
        cols, rows = slice(384 * g, 384 * (g + 1)), slice(8 * g, 8 * (g + 1))
        with jax.named_scope(f"w_att{g}"):
            drain(att.at[0, :, cols], recv_sem.at[5 + g])
        both = att[:, :, cols].reshape(256, 384)
        for t in range(0, 4, 2):
            got = lax.dot_general(
                both, cot[:, :, 128 * t : 128 * (t + 2)].reshape(256, 256), (((0,), (0,)), ((), ())),
                preferred_element_type=F32,
            )
            for k in range(2):
                terms[t + k, rows] = got[:, 128 * k : 128 * (k + 1)].astype(BF16).reshape(8, 2, 3, 8, 128)
        for d in (2, 1, 3):
            t, where = a_peer(d)
            send(terms.at[t, rows, c], across.at[d - 1, rows], 27 + g, 37 + g, where)

    crossed(4)
    attended = dot(att[c], order_out[...]).astype(BF16)
    for t in range(0, 4, 2):
        total = hidden[:, 128 * t : 128 * (t + 2)]
        for i in range(3):
            w = jnp.concatenate([unit(4 * i + t, 4), unit(4 * i + t + 1, 4)], axis=1)
            total = total + dot(attended[:, 256 * i : 256 * (i + 1)], w)
        layer[0, :, 128 * t : 128 * (t + 2)] = total.astype(BF16)

    for g in range(2):
        rows = slice(8 * g, 8 * (g + 1))
        with jax.named_scope(f"w_across{g}"):
            drain(across.at[:, rows], recv_sem.at[37 + g])
        total = terms[a, rows, c].astype(F32)
        for d in range(3):
            total = total + across[d, rows].astype(F32)
        summed[rows] = total.astype(BF16)

        def reduce_z(t, _):
            @pl.when(t != z)
            def _():
                send(summed.at[t], along.at[z], 29, 39, {"z": t})

            return 0

        lax.fori_loop(8 * g, 8 * (g + 1), reduce_z, 0)
    along[z] = summed[z]
    with jax.named_scope("w_along"):
        drain(along.at[0:15], recv_sem.at[39])
    total = along[0].astype(F32)
    for k in range(1, NZ):
        total = total + along[k].astype(F32)
    final[piece] = total.astype(BF16)

    def show(k, _):
        send(final.at[piece], final.at[piece], 30, 40, plane_peer(k))
        return 0

    lax.fori_loop(1, 16, show, 0)
    with jax.named_scope("w_final"):
        drain(final.at[0:15], recv_sem.at[40])
    factor = (16 * 4096) ** -0.5
    for t in range(4):
        total = final[t].astype(F32)
        for k in range(1, 4):
            total = total + final[4 * k + t].astype(F32)
        grad[:, 128 * t : 128 * (t + 1)] = total.reshape(24, 128) * factor

    drain(asked.at[0:31], send_sem.at[0])
    drain(cot.at[0], send_sem.at[1])
    drain(table.at[0:31], send_sem.at[2])
    drain(shorts.at[0, 0:15], send_sem.at[3])
    drain(shorts.at[0], send_sem.at[4])
    for n, (lo, hi, s0, s1) in enumerate(CHUNKS):
        drain(held.at[0, lo:hi, 0, max(s0, 1) : s1], send_sem.at[5 + n])
        drain(held.at[0:3, lo:hi, 0, s0:s1], send_sem.at[10 + n])
        drain(held.at[0:12, lo:hi, 0, s0:s1], send_sem.at[15 + n])
        drain(held.at[:, lo:hi, 0, s0:s1], send_sem.at[20 + n])
    for g in range(2):
        drain(att.at[0, :, 384 * g : 384 * (g + 1)], send_sem.at[25 + g])
        drain(across.at[:, 8 * g : 8 * (g + 1)], send_sem.at[27 + g])
    drain(along.at[0:15], send_sem.at[29])
    drain(final.at[0:15], send_sem.at[30])


def shards(feats, near_map, wanted, counts, choice, conv, gain, inw, outw, cot):
    vmem = pl.BlockSpec(memory_space=pltpu.VMEM)
    hbm = pl.BlockSpec(memory_space=pltpu.HBM)
    v = pltpu.VMEM
    return pl.pallas_call(
        kernel,
        name="layer",
        out_shape=(jax.ShapeDtypeStruct((1, 128, 512), BF16), jax.ShapeDtypeStruct((24, 512), F32)),
        in_specs=[hbm] * 10,
        out_specs=(vmem, vmem),
        scratch_shapes=[
            v((128, 256), BF16),
            v((6, 1, 128), jnp.int32),
            v((1, 1, 8, 32), jnp.int32),
            pltpu.SMEM((1, 32), jnp.int32),
            pltpu.SMEM((1, 2, 4), jnp.int32),
            v((1, 512), F32),
            v((2, 128, 128), F32),
            v((32, 1, 128), jnp.int32),
            v((32, 1, 128), jnp.int32),
            v((48, 8, 256), BF16),
            v((32, 8, 256), BF16),
            v((128, 256), BF16),
            v((768, 384), BF16),
            v((6, 128, 256), BF16),
            v((5, 8, 128), BF16),
            v((16, 5, 2, NZ, 8, 128), BF16),
            v((128, 512), F32),
            v((128, 2304), BF16),
            v((24, 128), F32),
            v((2, NZ, 3, 8, 128), BF16),
            v((96, 128), F32),
            v((6, 256, 128), BF16),
            v((6, 256, 128), F32),
            v((2, 128, 512), BF16),
            v((2, 128, 768), BF16),
            v((4, NZ, 2, 3, 8, 128), BF16),
            v((3, NZ, 3, 8, 128), BF16),
            v((NZ, 3, 8, 128), BF16),
            v((NZ, 3, 8, 128), BF16),
            v((16, 3, 8, 128), BF16),
            v((256, 256), BF16),
            v((512, 512), BF16),
            v((768, 768), BF16),
            pltpu.SemaphoreType.DMA((12,)),
            pltpu.SemaphoreType.DMA((31,)),
            pltpu.SemaphoreType.DMA((41,)),
        ],
        compiler_params=pltpu.CompilerParams(
            collective_id=0, has_side_effects=True, vmem_limit_bytes=VMEM
        ),
    )(
        *(
            pltpu.with_memory_space_constraint(array, pltpu.HBM)
            for array in (
                feats, near_map.transpose(2, 0, 1), wanted.swapaxes(2, 3), counts, choice, conv, gain.reshape(1, -1), inw, outw, cot
            )
        )
    )


def solution(mesh):
    space = ("z", "c")
    dp = ("y", "x")
    torus = Mesh(mesh.devices.reshape(4, 4, 16, 2), dp + space)
    return jax.shard_map(
        shards,
        mesh=torus,
        in_specs=(
            P(dp, space, None),
            P(dp, space, None),
            P(dp, space, None, None),
            P(dp, None),
            P(dp, space, None),
            P(None, space, None),
            P(),
            P(space, None),
            P(space, None),
            P(dp, space, None),
        ),
        out_specs=(P(dp, space, None), P(space, None)),
        check_vma=False,
    )
```

```python
import jax
import jax.numpy as jnp
from jax import lax
from jax.experimental import pallas as pl
from jax.experimental.pallas import tpu as pltpu
from jax.sharding import Mesh
from jax.sharding import PartitionSpec as P

MESH = pl.DeviceIdType.MESH
F32 = jnp.float32
BF16 = jnp.bfloat16
NZ = 16
VMEM = 48 * 1024 * 1024
CHUNKS = (
    (0, 2, 0, 8, 0), (0, 2, 8, 16, 0), (0, 2, 0, 8, 1), (0, 2, 8, 16, 1), (2, 4, 0, 16, 0), (2, 4, 0, 16, 1), (4, 5, 0, 16, 0)
)
RELAYED = (6,)


def iota(shape, dim):
    return lax.broadcasted_iota(jnp.int32, shape, dim)


def one_hot(flags):
    return jnp.where(flags, 1.0, 0.0).astype(BF16)


def ordering(parts, z):
    n = 256 * parts
    col = iota((1, n), 1)
    slot = (col >> 3) & 15
    chip = (z + NZ + jnp.where((slot & 1) == 1, (slot + 1) >> 1, -(slot >> 1))) & 15
    natural = chip * (16 * parts) + ((col >> 7) & 1) * (8 * parts) + (col >> 8) * 8 + (col & 7)
    return one_hot(iota((n, n), 0) == natural)


def dot(a, b):
    return jnp.dot(a, b, preferred_element_type=F32)


def dot_t(a, b):
    return lax.dot_general(a, b, (((1,), (1,)), ((), ())), preferred_element_type=F32)


def drain(ref, sem):
    pltpu.make_async_copy(ref, ref, sem).wait()


def kernel(
    feats_h, near_h, wanted_h, counts_h, choice_h, conv_h, gain_h, inw_h, outw_h, cot_h,
    layer, grad,
    feats, near_map, wanted, counts, choice, gain, turned,
    asked, asks, table, answers, own_feats, taps_hot, taps, staged, staged_far, held,
    hidden, qkv, tall, shorts, picked, split_q, scores, cot, att, terms, across, summed, along, final,
    order_taps, order_in, order_out,
    local_sem, send_sem, recv_sem,
):
    y, x, z, c = (lax.axis_index(n) for n in ("y", "x", "z", "c"))
    other = 1 - c
    me = z * 2 + c
    plane = y * 4 + x
    a = (1 - c) * x + c * y
    b = (1 - c) * y + c * x
    piece = b * 4 + a
    b_far = lax.rem(b + 2, 4)
    piece_far = b_far * 4 + a

    def z_of(slot):
        return lax.rem(z + NZ - (2 * lax.rem(slot, 2) - 1) * ((slot + 1) // 2), NZ)

    def a_peer(d):
        t = lax.rem(a + d, 4)
        return t, {"x": (1 - c) * t + c * x, "y": (1 - c) * y + c * t}

    def b_peer(d):
        t = lax.rem(b + d, 4)
        return t, {"x": (1 - c) * x + c * t, "y": (1 - c) * t + c * y}

    def plane_peer(k):
        t = lax.rem(plane + k, 16)
        return {"y": t // 4, "x": lax.rem(t, 4)}

    def send(src, dst, s, r, where):
        pltpu.make_async_remote_copy(
            src_ref=src, dst_ref=dst, send_sem=send_sem.at[s], recv_sem=recv_sem.at[r],
            device_id=where, device_id_type=MESH,
        ).start()

    def fetch(src, dst, k):
        copy = pltpu.make_async_copy(src, dst, local_sem.at[k])
        copy.start()
        return copy

    lanes = pl.ds(pl.multiple_of(a * 128, 128), 128)
    first = [
        fetch(wanted_h, wanted, 6),
        fetch(near_h, near_map, 7),
        fetch(feats_h.at[0], feats, 8),
    ]
    later = [
        fetch(counts_h, counts, 9),
        fetch(choice_h, choice, 10),
        fetch(gain_h, gain, 11),
    ]
    copies = [
        fetch(cot_h.at[0], cot.at[c], 0),
        fetch(conv_h.at[2 * b, :, lanes], staged.at[0], 1),
        fetch(conv_h.at[2 * b_far, :, lanes], staged_far.at[0], 12),
        fetch(inw_h.at[pl.ds(0, 8), pl.ds(pl.multiple_of(piece * 128, 128), 128)], staged.at[2], 3),
        fetch(inw_h.at[pl.ds(8, 8), pl.ds(pl.multiple_of(piece * 128, 128), 128)], staged.at[3], 4),
        fetch(outw_h.at[pl.ds(pl.multiple_of(lax.rem(b, 3) * 8, 8), 8), lanes], staged.at[4], 5),
        fetch(inw_h.at[pl.ds(0, 8), pl.ds(pl.multiple_of(piece_far * 128, 128), 128)], staged_far.at[2], 14),
        fetch(inw_h.at[pl.ds(8, 8), pl.ds(pl.multiple_of(piece_far * 128, 128), 128)], staged_far.at[3], 15),
    ]

    for k, (at, to) in enumerate(((b, staged), (b_far, staged_far))):

        @pl.when(at < 3)
        def _(k=k, at=at, to=to):
            fetch(conv_h.at[2 * at + 1, :, lanes], to.at[1], 2 + 11 * k)

        @pl.when(at == 3)
        def _(k=k, to=to):
            half_rows = pl.ds(pl.multiple_of(lax.rem(a, 2) * 8, 8), 8)
            fetch(inw_h.at[half_rows, pl.ds(pl.multiple_of((16 + a // 2) * 128, 128), 128)], to.at[1], 2 + 11 * k)

    barrier = pltpu.get_barrier_semaphore()

    def hail(where):
        pl.semaphore_signal(barrier, inc=1, device_id=where, device_id_type=MESH)

    def hail_z(i, _):
        hail({"z": z_of(i), "c": 0})
        hail({"z": z_of(i), "c": 1})
        return 0

    lax.fori_loop(1, NZ, hail_z, 0)
    lax.fori_loop(1, 16, lambda k, _: (hail(plane_peer(k)), 0)[1], 0)
    hail({"c": other})

    turned[...] = jnp.zeros_like(turned)
    for copy in first:
        copy.wait()
    turned[0, 0:8, 0:32] = wanted[0, 0].astype(F32)
    for k in range(6):
        turned[1, k : k + 1, :] = near_map[k].astype(F32)
    lists = turned[0].T.astype(jnp.int32)
    for p in range(32):
        asks[p] = lists[p : p + 1, :]
    asked[me] = asks[me]
    rows = turned[1].T
    for k in range(6):
        taps_hot[128 * k : 128 * (k + 1), :] = one_hot(rows[:, k : k + 1].astype(jnp.int32) == iota((128, 384), 1))
    order_taps[...] = ordering(1, z)
    ordered = dot(feats[...], order_taps[...]).astype(BF16)
    own_feats[...] = ordered
    table[0:16] = ordered.reshape(16, 8, 256)
    for copy in copies:
        copy.wait()
    drain(staged.at[1], local_sem.at[2])
    drain(staged_far.at[1], local_sem.at[13])
    held[piece, :, c, 0] = staged[...]
    held[piece_far, 0:4, c, 0] = staged_far[...]
    with jax.named_scope("w_barrier"):
        pl.semaphore_wait(barrier, 46)

    def far_first(body):
        lax.fori_loop(1, NZ, lambda i, _: (body(NZ - i), 0)[1], 0)

    def ask(slot):
        t = z_of(slot)
        for core in range(2):
            send(asks.at[t * 2 + core], asked.at[me], 0, 0, {"z": t, "c": core})

    def spread(n):
        lo, hi, s0, s1, far = CHUNKS[n]

        def one(slot, _):
            source, p = (staged_far.at[lo:hi], piece_far) if far else (staged.at[lo:hi], piece)
            send(source, held.at[p, lo:hi, c, slot], 5 + n, 7 + n, {"z": z_of(slot)})
            return 0

        lax.fori_loop(max(s0, 1), s1, one, 0)

    far_first(ask)
    send(asks.at[z * 2 + other], asked.at[me], 0, 0, {"c": other})
    for n in range(5):
        spread(n)
    send(cot.at[c], cot.at[c], 1, 1, {"c": other})
    for copy in later:
        copy.wait()
    order_in[...] = ordering(2, z)
    order_out[...] = ordering(3, z)

    def part(n, p, count, from_slot=None, to_slot=None):
        lo, hi, s0, s1, _ = CHUNKS[n]
        return held.at[pl.ds(p, count), lo:hi, c, s0 if from_slot is None else from_slot : s1 if to_slot is None else to_slot]

    def cross(n, p, count):
        some = part(n, p, count)
        send(some, some, 26 + n, 42 + n, {"c": other})

    def along_a(n):
        lo, hi, s0, s1, far = CHUNKS[n]
        with jax.named_scope(f"w_z{n}"):
            drain(held.at[0, lo:hi, 0, max(s0, 1) : s1], recv_sem.at[7 + n])
        some = part(n, piece_far if far else piece, 1)
        for d in (2, 1, 3):
            send(some, some, 12 + n, 14 + n, a_peer(d)[1])

    def along_b(n):
        lo, hi, s0, s1, far = CHUNKS[n]
        with jax.named_scope(f"w_a{n}"):
            drain(held.at[0:3, lo:hi, 0, s0:s1], recv_sem.at[14 + n])
        if not far:
            for k, d in enumerate((1, 3)):
                send(part(n, b * 4, 4), part(n, b * 4, 4), 19 + n, 21 + 7 * k + n, b_peer(d)[1])
        cross(n, (b_far if far else b) * 4, 4)

    def relay(n):
        lo, hi, s0, s1, _ = CHUNKS[n]
        middle = (s0 + s1) // 2
        for k, d, low, high in ((0, 1, s0, middle), (1, 3, middle, s1)):
            source = lax.rem(b + 4 - d, 4) * 4
            with jax.named_scope(f"w_b{n}"):
                drain(part(n, source, 4), recv_sem.at[21 + 7 * k + n])
            if n in RELAYED:
                send(part(n, source, 4, low, high), part(n, source, 4, low, high), 19 + n, 35 + n, b_peer(d)[1])
            cross(n, source, 4)

    def last(n):
        with jax.named_scope(f"w_f{n}"):
            drain(part(n, b_far * 4, 4), recv_sem.at[35 + n])
        cross(n, b_far * 4, 4)

    def crossings(n):
        return 16 if n in RELAYED else 4 if CHUNKS[n][4] else 12

    def crossed(n):
        lo, hi, s0, s1, _ = CHUNKS[n]
        with jax.named_scope(f"w_c{n}"):
            drain(held.at[0 : crossings(n), lo:hi, 0, s0:s1], recv_sem.at[42 + n])

    along_a(0)

    with jax.named_scope("w_ask"):
        drain(asked.at[0:31], recv_sem.at[0])
    lists = asked[:, 0, :].astype(F32).astype(BF16)
    spread_out = dot(one_hot((iota((256, 32), 0) >> 3) == iota((256, 32), 1)), lists)
    lane = iota((256, 128), 1)
    row = jnp.sum(jnp.where(lane == (iota((256, 128), 0) & 7), spread_out, 0.0), axis=1, keepdims=True)
    picked_rows = dot(one_hot(row == lane.astype(F32)), feats[...]).astype(BF16)
    answers[...] = picked_rows.reshape(32, 8, 256)
    table[16 + me] = answers[me]

    def answer(slot):
        t = z_of(slot)
        for core in range(2):
            send(answers.at[t * 2 + core], table.at[16 + me], 2, 2, {"z": t, "c": core})

    far_first(answer)
    send(answers.at[z * 2 + other], table.at[16 + me], 2, 2, {"c": other})
    spread(5)
    spread(6)

    along_b(0)
    along_a(1)
    along_a(2)
    along_a(3)
    along_b(1)
    relay(0)
    along_a(4)
    along_b(2)
    along_b(3)
    relay(1)
    with jax.named_scope("w_rows"):
        drain(table.at[0:31], recv_sem.at[2])
    fetched = table[16:48].reshape(256, 256)
    table[16:48] = dot(fetched, order_taps[...]).astype(BF16).reshape(32, 8, 256)
    for k in range(3):
        got = dot(taps_hot[256 * k : 256 * (k + 1), :], table[...].reshape(384, 256))
        taps[2 * k : 2 * k + 2] = got.astype(BF16).reshape(2, 128, 256)
    for n in range(4):
        crossed(n)
    along_b(4)

    def unit(p, u):
        return held[p, u].reshape(256, 128)

    count = counts[0, me]
    alive = jnp.where(iota((128, 128), 0) < count, 1.0, 0.0)
    alive_wide = jnp.concatenate([alive, alive], axis=1)
    for t in range(0, 4, 2):
        total = jnp.zeros((128, 256), F32)
        for k in range(7):
            p, u = (k // 2) * 4 + t, k % 2
            tap = own_feats[...] if k == 0 else taps[k - 1]
            total = total + dot(tap, jnp.concatenate([unit(p, u), unit(p + 1, u)], axis=1))
        hidden[:, 128 * t : 128 * (t + 2)] = total * alive_wide
    h = hidden[...]
    power = jnp.mean(h * h, axis=-1, keepdims=True)
    normed = (h * lax.rsqrt(power + 1e-06) * gain[...]).astype(BF16)

    token = iota((8, 128), 1)
    block_mask = one_hot(((token >> 6) == iota((8, 128), 0)) & (token < count))
    number = jnp.clip(count - 64 * iota((8, 1), 0), 0, 64)
    means = dot(block_mask, normed) / jnp.maximum(number, 1).astype(F32)
    for j in range(4):
        tall[2 * j : 2 * j + 2, :] = means[0:2, 128 * j : 128 * (j + 1)]
    shorts[me] = tall[...].astype(BF16)

    def tell(slot):
        for core in range(2):
            send(shorts.at[me], shorts.at[me], 3, 3, {"z": z_of(slot), "c": core})

    far_first(tell)
    send(shorts.at[me], shorts.at[me], 3, 3, {"c": other})

    normed = dot(normed, order_in[...]).astype(BF16)
    along_a(5)
    relay(4)
    along_b(5)
    along_a(6)
    crossed(4)
    crossed(5)

    def project(rows, j):
        upper, lower = [], []
        for t in (j, j + 1):
            if t < 16:
                upper.append(unit(t, 2))
                lower.append(unit(t, 3))
            else:
                upper.append(unit(12 + 2 * (t - 16), 1))
                lower.append(unit(13 + 2 * (t - 16), 1))
        got = dot(rows[:, :256], jnp.concatenate(upper, axis=1))
        return (got + dot(rows[:, 256:], jnp.concatenate(lower, axis=1))).astype(BF16)

    for j in range(0, 18, 2):
        qkv[:, 128 * j : 128 * (j + 2)] = project(normed, j)

    half = iota((128, 128), 1) < 64
    row256 = iota((256, 128), 0) & 127
    col256 = iota((256, 128), 1)
    near_ok = ((row256 >> 6) == (col256 >> 6)) & (col256 < count)
    for j in range(6):
        q = qkv[:, 128 * j : 128 * (j + 1)] * jnp.asarray(0.125, BF16)
        none = jnp.zeros_like(q)
        q = jnp.concatenate([jnp.where(half, q, none), jnp.where(half, none, q)], axis=0)
        split_q[j] = q
        scores[j] = jnp.where(near_ok, dot_t(q, qkv[:, 768 + 128 * j : 768 + 128 * (j + 1)]), -1e30)
    m32 = iota((32, 1), 0)
    target = jnp.zeros((32, 1), jnp.int32)
    for e in range(8):
        block = choice[0, e // 4, e % 4]
        target = jnp.where((m32 & 7) == e, (block // 2) * 8 + lax.rem(block, 2), target)
    chosen_hot = one_hot(target + 2 * (m32 >> 3) == iota((32, 256), 1))

    along_b(6)
    with jax.named_scope("w_short"):
        drain(shorts.at[0:31], recv_sem.at[3])
    chosen = dot(chosen_hot, shorts[...].reshape(256, 128))
    chosen = jnp.concatenate([chosen[8 * j : 8 * j + 8] for j in range(4)], axis=1).astype(BF16)
    chosen = dot(chosen, order_in[...]).astype(BF16)
    for j in range(6, 18, 2):
        picked[:, 128 * (j - 6) : 128 * (j - 4)] = project(chosen, j)
    far_ok = ((iota((256, 8), 0) & 127) >> 6) == (iota((256, 8), 1) >> 2)
    for j in range(6):
        near = scores[j]
        far = dot_t(split_q[j], picked[:, 128 * j : 128 * (j + 1)])
        far = jnp.where(far_ok, far, -1e30)
        top = jnp.maximum(jnp.max(near, axis=1, keepdims=True), jnp.max(far, axis=1, keepdims=True))
        near, far = jnp.exp(near - top), jnp.exp(far - top)
        scale = 1.0 / (jnp.sum(near, axis=1, keepdims=True) + jnp.sum(far, axis=1, keepdims=True))
        near, far = (near * scale).astype(BF16), (far * scale).astype(BF16)
        mixed = dot(near, qkv[:, 1536 + 128 * j : 1536 + 128 * (j + 1)])
        mixed = mixed + dot(far, picked[:, 768 + 128 * j : 768 + 128 * (j + 1)])
        mixed = jnp.where(half, mixed[:128], mixed[128:]) * alive
        att[c, :, 128 * j : 128 * (j + 1)] = mixed.astype(BF16)
        if j % 3 == 2:
            part_of = att.at[c, :, 128 * (j - 2) : 128 * (j + 1)]
            send(part_of, part_of, 33 + j // 3, 5 + j // 3, {"c": other})

    drain(cot.at[0], recv_sem.at[1])
    for g in range(2):
        cols, rows = slice(384 * g, 384 * (g + 1)), slice(8 * g, 8 * (g + 1))
        with jax.named_scope(f"w_att{g}"):
            drain(att.at[0, :, cols], recv_sem.at[5 + g])
        both = att[:, :, cols].reshape(256, 384)
        for t in range(0, 4, 2):
            got = lax.dot_general(
                both, cot[:, :, 128 * t : 128 * (t + 2)].reshape(256, 256), (((0,), (0,)), ((), ())),
                preferred_element_type=F32,
            )
            for k in range(2):
                terms[t + k, rows] = got[:, 128 * k : 128 * (k + 1)].astype(BF16).reshape(8, 2, 3, 8, 128)
        for d in (2, 1, 3):
            t, where = a_peer(d)
            send(terms.at[t, rows, c], across.at[d - 1, rows], 35 + g, 49 + g, where)

    relay(6)
    for g in range(2):
        rows = slice(8 * g, 8 * (g + 1))
        with jax.named_scope(f"w_across{g}"):
            drain(across.at[:, rows], recv_sem.at[49 + g])
        total = terms[a, rows, c].astype(F32)
        for d in range(3):
            total = total + across[d, rows].astype(F32)
        summed[rows] = total.astype(BF16)

        def reduce_z(t, _):
            @pl.when(t != z)
            def _():
                send(summed.at[t], along.at[z], 37, 51, {"z": t})

            return 0

        lax.fori_loop(8 * g, 8 * (g + 1), reduce_z, 0)
    along[z] = summed[z]

    last(6)
    crossed(6)
    attended = dot(att[c], order_out[...]).astype(BF16)
    for t in range(0, 4, 2):
        total = hidden[:, 128 * t : 128 * (t + 2)]
        for i in range(3):
            w = jnp.concatenate([unit(4 * i + t, 4), unit(4 * i + t + 1, 4)], axis=1)
            total = total + dot(attended[:, 256 * i : 256 * (i + 1)], w)
        layer[0, :, 128 * t : 128 * (t + 2)] = total.astype(BF16)

    with jax.named_scope("w_along"):
        drain(along.at[0:15], recv_sem.at[51])
    total = along[0].astype(F32)
    for k in range(1, NZ):
        total = total + along[k].astype(F32)
    final[piece] = total.astype(BF16)

    def show(k, _):
        send(final.at[piece], final.at[piece], 38, 52, plane_peer(k))
        return 0

    lax.fori_loop(1, 16, show, 0)
    with jax.named_scope("w_final"):
        drain(final.at[0:15], recv_sem.at[52])
    factor = (16 * 4096) ** -0.5
    for t in range(4):
        total = final[t].astype(F32)
        for k in range(1, 4):
            total = total + final[4 * k + t].astype(F32)
        grad[:, 128 * t : 128 * (t + 1)] = total.reshape(24, 128) * factor

    drain(asked.at[0:31], send_sem.at[0])
    drain(cot.at[0], send_sem.at[1])
    drain(table.at[0:31], send_sem.at[2])
    drain(shorts.at[0:31], send_sem.at[3])
    for n, (lo, hi, s0, s1, far) in enumerate(CHUNKS):
        drain(held.at[0, lo:hi, 0, max(s0, 1) : s1], send_sem.at[5 + n])
        drain(held.at[0:3, lo:hi, 0, s0:s1], send_sem.at[12 + n])
        if not far:
            drain(held.at[0 : 12 if n in RELAYED else 8, lo:hi, 0, s0:s1], send_sem.at[19 + n])
        drain(held.at[0 : crossings(n), lo:hi, 0, s0:s1], send_sem.at[26 + n])
    for g in range(2):
        drain(att.at[0, :, 384 * g : 384 * (g + 1)], send_sem.at[33 + g])
        drain(across.at[:, 8 * g : 8 * (g + 1)], send_sem.at[35 + g])
    drain(along.at[0:15], send_sem.at[37])
    drain(final.at[0:15], send_sem.at[38])


def shards(feats, near_map, wanted, counts, choice, conv, gain, inw, outw, cot):
    vmem = pl.BlockSpec(memory_space=pltpu.VMEM)
    hbm = pl.BlockSpec(memory_space=pltpu.HBM)
    v = pltpu.VMEM
    return pl.pallas_call(
        kernel,
        name="layer",
        out_shape=(jax.ShapeDtypeStruct((1, 128, 512), BF16), jax.ShapeDtypeStruct((24, 512), F32)),
        in_specs=[hbm] * 10,
        out_specs=(vmem, vmem),
        scratch_shapes=[
            v((128, 256), BF16),
            v((6, 1, 128), jnp.int32),
            v((1, 1, 8, 32), jnp.int32),
            pltpu.SMEM((1, 32), jnp.int32),
            pltpu.SMEM((1, 2, 4), jnp.int32),
            v((1, 512), F32),
            v((2, 128, 128), F32),
            v((32, 1, 128), jnp.int32),
            v((32, 1, 128), jnp.int32),
            v((48, 8, 256), BF16),
            v((32, 8, 256), BF16),
            v((128, 256), BF16),
            v((768, 384), BF16),
            v((6, 128, 256), BF16),
            v((5, 8, 128), BF16),
            v((4, 8, 128), BF16),
            v((16, 5, 2, NZ, 8, 128), BF16),
            v((128, 512), F32),
            v((128, 2304), BF16),
            v((8, 128), F32),
            v((32, 8, 128), BF16),
            v((8, 1536), BF16),
            v((6, 256, 128), BF16),
            v((6, 256, 128), F32),
            v((2, 128, 512), BF16),
            v((2, 128, 768), BF16),
            v((4, NZ, 2, 3, 8, 128), BF16),
            v((3, NZ, 3, 8, 128), BF16),
            v((NZ, 3, 8, 128), BF16),
            v((NZ, 3, 8, 128), BF16),
            v((16, 3, 8, 128), BF16),
            v((256, 256), BF16),
            v((512, 512), BF16),
            v((768, 768), BF16),
            pltpu.SemaphoreType.DMA((16,)),
            pltpu.SemaphoreType.DMA((39,)),
            pltpu.SemaphoreType.DMA((53,)),
        ],
        compiler_params=pltpu.CompilerParams(
            collective_id=0, has_side_effects=True, vmem_limit_bytes=VMEM
        ),
    )(
        *(
            pltpu.with_memory_space_constraint(array, pltpu.HBM)
            for array in (
                feats, near_map.transpose(2, 0, 1), wanted.swapaxes(2, 3), counts, choice, conv, gain.reshape(1, -1), inw, outw, cot
            )
        )
    )


def solution(mesh):
    space = ("z", "c")
    dp = ("y", "x")
    torus = Mesh(mesh.devices.reshape(4, 4, 16, 2), dp + space)
    return jax.shard_map(
        shards,
        mesh=torus,
        in_specs=(
            P(dp, space, None),
            P(dp, space, None),
            P(dp, space, None, None),
            P(dp, None),
            P(dp, space, None),
            P(None, space, None),
            P(),
            P(space, None),
            P(space, None),
            P(dp, space, None),
        ),
        out_specs=(P(dp, space, None), P(space, None)),
        check_vma=False,
    )
```

```python
import jax
import jax.numpy as jnp
from jax import lax
from jax.experimental import pallas as pl
from jax.experimental.pallas import tpu as pltpu
from jax.sharding import Mesh
from jax.sharding import PartitionSpec as P

MESH = pl.DeviceIdType.MESH
F32 = jnp.float32
BF16 = jnp.bfloat16
NZ = 16
VMEM = 48 * 1024 * 1024
CHUNKS = {0: (0, 2, 0, 8, 0), 1: (0, 2, 8, 16, 0), 2: (0, 2, 0, 8, 1), 3: (0, 2, 8, 16, 1), 7: (2, 3, 0, 16, 0)}
RELAYED = (7,)
SPLIT = {4: (0, 8, 0), 5: (8, 16, 0), 6: (0, 16, 1)}


def iota(shape, dim):
    return lax.broadcasted_iota(jnp.int32, shape, dim)


def one_hot(flags):
    return jnp.where(flags, 1.0, 0.0).astype(BF16)


def ordering(parts, z):
    n = 256 * parts
    col = iota((1, n), 1)
    slot = (col >> 3) & 15
    chip = (z + NZ + jnp.where((slot & 1) == 1, (slot + 1) >> 1, -(slot >> 1))) & 15
    natural = chip * (16 * parts) + ((col >> 7) & 1) * (8 * parts) + (col >> 8) * 8 + (col & 7)
    return one_hot(iota((n, n), 0) == natural)


def dot(a, b):
    return jnp.dot(a, b, preferred_element_type=F32)


def dot_t(a, b):
    return lax.dot_general(a, b, (((1,), (1,)), ((), ())), preferred_element_type=F32)


def turned_dot(a, b):
    return lax.dot_general(a, b, (((0,), (0,)), ((), ())), preferred_element_type=F32)


def drain(ref, sem):
    pltpu.make_async_copy(ref, ref, sem).wait()


def kernel(
    feats_h, near_h, wanted_h, counts_h, choice_h, conv_h, gain_h, inw_h, outw_h, cot_h,
    layer, grad,
    feats, near_map, wanted, counts, choice, gain, turned,
    asked, asks, table, answers, own_feats, taps_hot, taps, staged, staged_far, staged_in, held, split_in,
    hidden, normed_all, qkv, tall, shorts, chosen_hot, picked, split_q, near_mix, near_top, near_sum, cot, att, att_all, terms, across, summed, along, final,
    order_taps, order_in, order_out,
    local_sem, send_sem, recv_sem,
):
    y, x, z, c = (lax.axis_index(n) for n in ("y", "x", "z", "c"))
    other = 1 - c
    me = z * 2 + c
    plane = y * 4 + x
    a = (1 - c) * x + c * y
    b = (1 - c) * y + c * x
    piece = b * 4 + a
    b_far = lax.rem(b + 2, 4)
    piece_far = b_far * 4 + a
    core_pieces = ((y * 4 + x, lax.rem(y + 2, 4) * 4 + x), (x * 4 + y, lax.rem(x + 2, 4) * 4 + y))

    def z_of(slot):
        return lax.rem(z + NZ - (2 * lax.rem(slot, 2) - 1) * ((slot + 1) // 2), NZ)

    def a_peer(d):
        t = lax.rem(a + d, 4)
        return t, {"x": (1 - c) * t + c * x, "y": (1 - c) * y + c * t}

    def b_peer(d):
        t = lax.rem(b + d, 4)
        return t, {"x": (1 - c) * x + c * t, "y": (1 - c) * t + c * y}

    def plane_peer(k):
        t = lax.rem(plane + k, 16)
        return {"y": t // 4, "x": lax.rem(t, 4)}

    def send(src, dst, s, r, where):
        pltpu.make_async_remote_copy(
            src_ref=src, dst_ref=dst, send_sem=send_sem.at[s], recv_sem=recv_sem.at[r],
            device_id=where, device_id_type=MESH,
        ).start()

    def fetch(src, dst, k):
        copy = pltpu.make_async_copy(src, dst, local_sem.at[k])
        copy.start()
        return copy

    first = [
        fetch(wanted_h, wanted, 6),
        fetch(near_h, near_map, 7),
        fetch(feats_h.at[0], feats, 8),
    ]

    barrier = pltpu.get_barrier_semaphore()

    def hail(where):
        pl.semaphore_signal(barrier, inc=1, device_id=where, device_id_type=MESH)

    def hail_z(i, _):
        hail({"z": z_of(i), "c": 0})
        hail({"z": z_of(i), "c": 1})
        return 0

    lax.fori_loop(1, NZ, lambda i, _: hail_z(NZ - i, _), 0)
    lax.fori_loop(1, 16, lambda k, _: (hail(plane_peer(k)), 0)[1], 0)
    hail({"c": other})

    lanes = pl.ds(pl.multiple_of(a * 128, 128), 128)
    later = [
        fetch(counts_h, counts, 9),
        fetch(choice_h, choice, 10),
        fetch(gain_h, gain, 11),
    ]
    copies = [
        fetch(cot_h.at[0], cot.at[c], 0),
        fetch(conv_h.at[2 * b, :, lanes], staged.at[0], 1),
        fetch(conv_h.at[2 * b_far, :, lanes], staged_far.at[0], 12),
        fetch(outw_h.at[pl.ds(pl.multiple_of(lax.rem(b, 3) * 8, 8), 8), lanes], staged.at[2], 5),
        *(
            fetch(
                inw_h.at[
                    pl.ds(pl.multiple_of(lax.rem(p, 2) * 8, 8), 8),
                    pl.ds(pl.multiple_of((p // 6 * 6 + 3 * h + lax.rem(p // 2, 3)) * 128, 128), 128),
                ],
                staged_in.at[h, far], 16 + 2 * h + far,
            )
            for h in range(2) for far, p in enumerate(core_pieces[h])
        ),
    ]

    for k, (at, to) in enumerate(((b, staged), (b_far, staged_far))):

        @pl.when(at < 3)
        def _(k=k, at=at, to=to):
            fetch(conv_h.at[2 * at + 1, :, lanes], to.at[1], 2 + 11 * k)

        @pl.when(at == 3)
        def _(k=k, to=to):
            half_rows = pl.ds(pl.multiple_of(lax.rem(a, 2) * 8, 8), 8)
            fetch(inw_h.at[half_rows, pl.ds(pl.multiple_of((14 + 3 * (a // 2)) * 128, 128), 128)], to.at[1], 2 + 11 * k)

    turned[...] = jnp.zeros_like(turned)
    for copy in first:
        copy.wait()
    turned[0, 0:8, 0:32] = wanted[0, 0].astype(F32)
    for k in range(6):
        turned[1, k : k + 1, :] = near_map[k].astype(F32)
    lists = turned[0].T[0:32].astype(jnp.int32)
    slots = jnp.zeros((32, 128), jnp.int32)
    for k in range(8):
        slots = slots + jnp.where(lists[:, k : k + 1] == iota((32, 128), 1), 1 << k, 0)
    for p in range(32):
        asks[p] = slots[p : p + 1, :]
    asked[me] = asks[me]
    rows = turned[1].T
    for k in range(6):
        taps_hot[128 * k : 128 * (k + 1), :] = one_hot(rows[:, k : k + 1].astype(jnp.int32) == iota((128, 384), 1))
    order_taps[...] = ordering(1, z)
    ordered = dot(feats[...], order_taps[...]).astype(BF16)
    own_feats[...] = ordered
    table[0:16] = ordered.reshape(16, 8, 256)
    for copy in copies:
        copy.wait()
    drain(staged.at[1], local_sem.at[2])
    drain(staged_far.at[1], local_sem.at[13])
    held[piece, :, c, 0] = staged[...]
    held[piece_far, 0:2, c, 0] = staged_far[...]
    split_in[piece, c, 0] = staged_in[c, 0]
    split_in[piece_far, c, 0] = staged_in[c, 1]
    with jax.named_scope("w_barrier"):
        pl.semaphore_wait(barrier, 46)

    def far_first(body):
        lax.fori_loop(1, NZ, lambda i, _: (body(NZ - i), 0)[1], 0)

    def ask(slot):
        t = z_of(slot)
        for core in range(2):
            send(asks.at[t * 2 + core], asked.at[me], 0, 0, {"z": t, "c": core})

    def spread(n):
        lo, hi, s0, s1, far = CHUNKS[n]

        def one(slot, _):
            source, p = (staged_far.at[lo:hi], piece_far) if far else (staged.at[lo:hi], piece)
            send(source, held.at[p, lo:hi, c, slot], 5 + n, 7 + n, {"z": z_of(slot)})
            return 0

        lax.fori_loop(max(s0, 1), s1, one, 0)

    def spread_in(n):
        s0, s1, far = SPLIT[n]

        def one(slot, _):
            for h in range(2):
                send(staged_in.at[h, far], split_in.at[core_pieces[h][far], c, slot], 5 + n, 7 + n, {"z": z_of(slot), "c": h})
            return 0

        if s0 == 0:
            p = (1 - other) * core_pieces[0][far] + other * core_pieces[1][far]
            send(staged_in.at[other, far], split_in.at[p, c, 0], 5 + n, 7 + n, {"c": other})
        lax.fori_loop(max(s0, 1), s1, one, 0)

    def arrivals(n):
        return (split_in.at[0, 0, 0:15], split_in.at[0, 0], shorts.at[0:31])[n - 4]

    far_first(ask)
    send(asks.at[z * 2 + other], asked.at[me], 0, 0, {"c": other})
    for n in range(4):
        spread(n)
    spread_in(4)
    spread_in(5)
    send(cot.at[c], cot.at[c], 1, 1, {"c": other})
    for copy in later:
        copy.wait()
    m32 = iota((32, 1), 0)
    target = jnp.zeros((32, 1), jnp.int32)
    for e in range(8):
        block = choice[0, e // 4, e % 4]
        target = jnp.where((m32 & 7) == e, (block // 2) * 8 + lax.rem(block, 2), target)
    chosen_hot[c] = one_hot(target + 2 * (m32 >> 3) == iota((32, 256), 1))
    order_in[...] = ordering(2, z)
    order_out[...] = ordering(3, z)

    def part(n, p, count, from_slot=None, to_slot=None):
        lo, hi, s0, s1, _ = CHUNKS[n]
        return held.at[pl.ds(p, count), lo:hi, c, s0 if from_slot is None else from_slot : s1 if to_slot is None else to_slot]

    def cross(n, p, count):
        some = part(n, p, count)
        send(some, some, 29 + n, 47 + n, {"c": other})

    def along_a(n):
        lo, hi, s0, s1, far = CHUNKS[n]
        with jax.named_scope(f"w_z{n}"):
            drain(held.at[0, lo:hi, 0, max(s0, 1) : s1], recv_sem.at[7 + n])
        some = part(n, piece_far if far else piece, 1)
        for d in (2, 1, 3):
            send(some, some, 13 + n, 15 + n, a_peer(d)[1])

    def along_b(n):
        lo, hi, s0, s1, far = CHUNKS[n]
        with jax.named_scope(f"w_a{n}"):
            drain(held.at[0:3, lo:hi, 0, s0:s1], recv_sem.at[15 + n])
        if not far:
            for k, d in enumerate((1, 3)):
                send(part(n, b * 4, 4), part(n, b * 4, 4), 21 + n, 23 + 8 * k + n, b_peer(d)[1])
        cross(n, (b_far if far else b) * 4, 4)

    def relay(n):
        lo, hi, s0, s1, _ = CHUNKS[n]
        middle = (s0 + s1) // 2
        for k, d, low, high in ((0, 1, s0, middle), (1, 3, middle, s1)):
            source = lax.rem(b + 4 - d, 4) * 4
            with jax.named_scope(f"w_b{n}"):
                drain(part(n, source, 4), recv_sem.at[23 + 8 * k + n])
            if n in RELAYED:
                send(part(n, source, 4, low, high), part(n, source, 4, low, high), 21 + n, 39 + n, b_peer(d)[1])
            cross(n, source, 4)

    def last(n):
        with jax.named_scope(f"w_f{n}"):
            drain(part(n, b_far * 4, 4), recv_sem.at[39 + n])
        cross(n, b_far * 4, 4)

    def part_in(n, p, count):
        s0, s1, _ = SPLIT[n]
        return split_in.at[pl.ds(p, count), :, s0:s1]

    def split_a(n):
        with jax.named_scope(f"w_z{n}"):
            drain(arrivals(n), recv_sem.at[7 + n])
        some = part_in(n, piece_far if SPLIT[n][2] else piece, 1)
        for d in (2, 1, 3):
            send(some, some, 13 + n, 15 + n, a_peer(d)[1])

    def split_b(n):
        with jax.named_scope(f"w_a{n}"):
            drain(part_in(n, 0, 3), recv_sem.at[15 + n])
        if not SPLIT[n][2]:
            for k, d in enumerate((1, 3)):
                send(part_in(n, b * 4, 4), part_in(n, b * 4, 4), 21 + n, 23 + 8 * k + n, b_peer(d)[1])

    def split_end(n):
        for k, d in ((0, 1), (1, 3)):
            with jax.named_scope(f"w_b{n}"):
                drain(part_in(n, lax.rem(b + 4 - d, 4) * 4, 4), recv_sem.at[23 + 8 * k + n])

    def crossings(n):
        return 16 if n in RELAYED else 4 if CHUNKS[n][4] else 12

    def crossed(n):
        lo, hi, s0, s1, _ = CHUNKS[n]
        with jax.named_scope(f"w_c{n}"):
            drain(held.at[0 : crossings(n), lo:hi, 0, s0:s1], recv_sem.at[47 + n])

    send(chosen_hot.at[c], chosen_hot.at[c], 4, 4, {"c": other})
    along_a(0)

    with jax.named_scope("w_ask"):
        drain(asked.at[0:31], recv_sem.at[0])
    wants = jnp.broadcast_to(asked[...], (32, 8, 128))
    wants = one_hot(((wants >> iota((32, 8, 128), 1)) & 1) == 1).reshape(256, 128)
    picked_rows = dot(wants, feats[...]).astype(BF16)
    answers[...] = picked_rows.reshape(32, 8, 256)
    table[16 + me] = answers[me]

    def answer(slot):
        t = z_of(slot)
        for core in range(2):
            send(answers.at[t * 2 + core], table.at[16 + me], 2, 2, {"z": t, "c": core})

    far_first(answer)
    send(answers.at[z * 2 + other], table.at[16 + me], 2, 2, {"c": other})
    spread_in(6)
    spread(7)

    along_a(1)
    along_b(0)
    along_a(2)
    along_a(3)
    along_b(1)
    relay(0)
    split_a(4)
    split_a(5)
    along_b(2)
    along_b(3)
    relay(1)
    with jax.named_scope("w_rows"):
        drain(table.at[0:31], recv_sem.at[2])
    fetched = table[16:48].reshape(256, 256)
    table[16:48] = dot(fetched, order_taps[...]).astype(BF16).reshape(32, 8, 256)
    for k in range(3):
        got = dot(taps_hot[256 * k : 256 * (k + 1), :], table[...].reshape(384, 256))
        taps[2 * k : 2 * k + 2] = got.astype(BF16).reshape(2, 128, 256)
    split_b(4)
    for n in range(4):
        crossed(n)
    split_b(5)

    def unit(p, u):
        return held[p, u].reshape(256, 128)

    count = counts[0, me]
    alive = jnp.where(iota((128, 128), 0) < count, 1.0, 0.0)
    alive_wide = jnp.concatenate([alive, alive], axis=1)
    for t in range(0, 4, 2):
        total = jnp.zeros((128, 256), F32)
        for k in range(7):
            p, u = (k // 2) * 4 + t, k % 2
            tap = own_feats[...] if k == 0 else taps[k - 1]
            total = total + dot(tap, jnp.concatenate([unit(p, u), unit(p + 1, u)], axis=1))
        hidden[:, 128 * t : 128 * (t + 2)] = total * alive_wide
    h = hidden[...]
    power = jnp.mean(h * h, axis=-1, keepdims=True)
    normed = (h * lax.rsqrt(power + 1e-06) * gain[...]).astype(BF16)

    token = iota((8, 128), 1)
    block_mask = one_hot(((token >> 6) == iota((8, 128), 0)) & (token < count))
    number = jnp.clip(count - 64 * iota((8, 1), 0), 0, 64)
    means = dot(block_mask, normed) / jnp.maximum(number, 1).astype(F32)
    for j in range(4):
        tall[2 * j : 2 * j + 2, :] = means[0:2, 128 * j : 128 * (j + 1)]
    shorts[me] = tall[...].astype(BF16)

    def tell(slot):
        for core in range(2):
            send(shorts.at[me], shorts.at[me], 3, 3, {"z": z_of(slot), "c": core})

    far_first(tell)
    send(shorts.at[me], shorts.at[me], 3, 3, {"c": other})

    normed_all[c] = dot(normed, order_in[...]).astype(BF16)
    send(normed_all.at[c], normed_all.at[c], 38, 6, {"c": other})
    split_a(6)
    split_end(4)
    along_a(7)
    with jax.named_scope("w_norm"):
        drain(normed_all.at[0], recv_sem.at[6])
    split_end(5)
    split_b(6)

    def unit_in(tile, i):
        if tile < 8:
            return split_in[2 * tile + i].reshape(256, 128)
        return held[12 + 2 * c + i, 1].reshape(256, 128)

    def project(rows, tiles):
        upper = jnp.concatenate([unit_in(t, 0) for t in tiles], axis=1)
        lower = jnp.concatenate([unit_in(t, 1) for t in tiles], axis=1)
        return dot(rows[:, :256], upper) + dot(rows[:, 256:], lower)

    tokens = normed_all[...].reshape(256, 512)
    for tiles in ((0, 1), (2, 3), (4, 5), (6, 7), (8,)):
        qkv[:, 128 * tiles[0] : 128 * (tiles[-1] + 1)] = project(tokens, tiles).astype(BF16)

    half = iota((128, 128), 1) < 64
    key = iota((128, 256), 0)
    same_block = (key >> 6) == ((iota((128, 256), 1) & 127) >> 6)
    for core in range(2):
        near_ok = same_block & (key < counts[0, 2 * z + core])
        rows = slice(128 * core, 128 * (core + 1))
        for j in range(3):
            at = 3 * core + j
            q = qkv[rows, 128 * j : 128 * (j + 1)] * jnp.asarray(0.125, BF16)
            none = jnp.zeros_like(q)
            q = jnp.concatenate([jnp.where(half, q, none), jnp.where(half, none, q)], axis=0)
            split_q[at] = q
            near = jnp.where(near_ok, dot_t(qkv[rows, 384 + 128 * j : 384 + 128 * (j + 1)], q), -1e30)
            top = jnp.max(near, axis=0, keepdims=True)
            near = jnp.exp(near - top)
            near_top[at] = top
            near_sum[at] = jnp.sum(near, axis=0, keepdims=True)
            mixed = turned_dot(qkv[rows, 768 + 128 * j : 768 + 128 * (j + 1)], near.astype(BF16))
            near_mix[at, 0:64] = mixed[0:64, 0:128]
            near_mix[at, 64:128] = mixed[64:128, 128:256]
    drain(chosen_hot.at[0], recv_sem.at[4])
    drain(cot.at[0], recv_sem.at[1])

    with jax.named_scope("w_short"):
        drain(shorts.at[0:31], recv_sem.at[3])
    chosen = dot(chosen_hot[...].reshape(64, 256), shorts[...].reshape(256, 128))
    chosen = jnp.concatenate(
        [jnp.concatenate([chosen[32 * k + 8 * j : 32 * k + 8 * j + 8] for j in range(4)], axis=1) for k in range(2)], axis=0
    ).astype(BF16)
    chosen = dot(chosen, order_in[...]).astype(BF16)
    for tiles in ((3, 4), (5, 6), (7, 8)):
        got = project(chosen, tiles)
        for k in range(2):
            picked[k, :, 128 * (tiles[0] - 3) : 128 * (tiles[0] - 1)] = got[8 * k : 8 * k + 8].astype(BF16)
    far_ok = (iota((8, 256), 0) >> 2) == ((iota((8, 256), 1) & 127) >> 6)
    for j in range(3):
        for core in range(2):
            at = 3 * core + j
            alive_row = jnp.where(iota((1, 128), 1) < counts[0, 2 * z + core], 1.0, 0.0)
            far = jnp.where(far_ok, dot_t(picked[core, :, 128 * j : 128 * (j + 1)], split_q[at]), -1e30)
            top = jnp.maximum(near_top[at], jnp.max(far, axis=0, keepdims=True))
            keep, far = jnp.exp(near_top[at] - top), jnp.exp(far - top)
            scale = 1.0 / (near_sum[at] * keep + jnp.sum(far, axis=0, keepdims=True))
            mixed = turned_dot(picked[core, :, 384 + 128 * j : 384 + 128 * (j + 1)], far.astype(BF16))
            for k in range(2):
                rows, cols = slice(64 * k, 64 * (k + 1)), slice(128 * k, 128 * (k + 1))
                both = near_mix[at, rows] * keep[:, cols] + mixed[rows, cols]
                att[core, 128 * j + 64 * k : 128 * j + 64 * (k + 1)] = (both * (scale[:, cols] * alive_row)).astype(BF16)
        if j == 0:
            continue
        g = j - 1
        rows = slice(192 * g, 192 * (g + 1))
        both = jnp.concatenate([att[0, rows], att[1, rows]], axis=1)
        for t in range(0, 4, 2):
            got = dot(both, cot[:, :, 128 * t : 128 * (t + 2)].reshape(256, 256))
            for k in range(2):
                terms[t + k, 4 * g : 4 * g + 4] = got[:, 128 * k : 128 * (k + 1)].astype(BF16).reshape(4, 2, 3, 8, 128)
        for d in (2, 1, 3):
            t, where = a_peer(d)
            send(terms.at[t, 4 * g : 4 * g + 4], across.at[d - 1, 4 * g : 4 * g + 4], 39 + g, 55 + g, where)
    att_all[c] = att[c]
    send(att.at[other], att_all.at[c], 37, 5, {"c": other})
    along_b(7)

    for g in range(2):
        rows = slice(4 * g, 4 * (g + 1))
        with jax.named_scope(f"w_across{g}"):
            drain(across.at[:, rows], recv_sem.at[55 + g])
        total = terms[a, rows].astype(F32)
        for d in range(3):
            total = total + across[d, rows].astype(F32)
        summed[rows] = total.astype(BF16)

        def reduce_z(k, _):
            for core in range(2):

                @pl.when((8 * c + k) * 2 + core != me)
                def _():
                    send(summed.at[k, core], along.at[z], 41, 57, {"z": 8 * c + k, "c": core})

            return 0

        lax.fori_loop(4 * g, 4 * (g + 1), reduce_z, 0)
    mine = z // 8 == c

    @pl.when(mine)
    def _():
        along[z] = summed[z - 8 * c, c]

    relay(7)
    with jax.named_scope("w_along"):

        @pl.when(mine)
        def _():
            drain(along.at[0:15], recv_sem.at[57])

        @pl.when(jnp.logical_not(mine))
        def _():
            drain(along, recv_sem.at[57])

    total = along[0].astype(F32)
    for k in range(1, NZ):
        total = total + along[k].astype(F32)
    sender = z // 8
    summed_piece = (1 - sender) * core_pieces[0][0] + sender * core_pieces[1][0]
    final[summed_piece] = total.astype(BF16)

    def show(k, _):
        send(final.at[summed_piece], final.at[summed_piece], 42, 58, plane_peer(k))
        return 0

    lax.fori_loop(1, 16, show, 0)
    last(7)
    crossed(7)
    drain(att_all.at[0], recv_sem.at[5])
    attended = turned_dot(att_all[...].reshape(768, 128), order_out[...]).astype(BF16)
    for t in range(0, 4, 2):
        total = hidden[:, 128 * t : 128 * (t + 2)]
        for i in range(3):
            w = jnp.concatenate([unit(4 * i + t, 2), unit(4 * i + t + 1, 2)], axis=1)
            total = total + dot(attended[:, 256 * i : 256 * (i + 1)], w)
        layer[0, :, 128 * t : 128 * (t + 2)] = total.astype(BF16)

    drain(asked.at[0:31], send_sem.at[0])
    drain(cot.at[0], send_sem.at[1])
    drain(table.at[0:31], send_sem.at[2])
    drain(shorts.at[0:31], send_sem.at[3])
    for n, (lo, hi, s0, s1, far) in CHUNKS.items():
        drain(held.at[0, lo:hi, 0, max(s0, 1) : s1], send_sem.at[5 + n])
        drain(held.at[0:3, lo:hi, 0, s0:s1], send_sem.at[13 + n])
        if not far:
            drain(held.at[0 : 12 if n in RELAYED else 8, lo:hi, 0, s0:s1], send_sem.at[21 + n])
        drain(held.at[0 : crossings(n), lo:hi, 0, s0:s1], send_sem.at[29 + n])
    for n, (s0, s1, far) in SPLIT.items():
        drain(arrivals(n), send_sem.at[5 + n])
        drain(part_in(n, 0, 3), send_sem.at[13 + n])
        if not far:
            drain(part_in(n, 0, 8), send_sem.at[21 + n])
    drain(chosen_hot.at[0], send_sem.at[4])
    drain(normed_all.at[0], send_sem.at[38])
    drain(att_all.at[0], send_sem.at[37])
    for g in range(2):
        drain(across.at[:, 4 * g : 4 * (g + 1)], send_sem.at[39 + g])

    with jax.named_scope("w_final"):
        drain(final.at[0:15], recv_sem.at[58])
    factor = (16 * 4096) ** -0.5
    for t in range(4):
        total = final[t].astype(F32)
        for k in range(1, 4):
            total = total + final[4 * k + t].astype(F32)
        grad[:, 128 * t : 128 * (t + 1)] = total.reshape(24, 128) * factor


    @pl.when(mine)
    def _():
        drain(along.at[0:15], send_sem.at[41])

    @pl.when(jnp.logical_not(mine))
    def _():
        drain(along, send_sem.at[41])

    drain(final.at[0:15], send_sem.at[42])


def shards(feats, near_map, wanted, counts, choice, conv, gain, inw, outw, cot):
    vmem = pl.BlockSpec(memory_space=pltpu.VMEM)
    hbm = pl.BlockSpec(memory_space=pltpu.HBM)
    v = pltpu.VMEM
    return pl.pallas_call(
        kernel,
        name="layer",
        out_shape=(jax.ShapeDtypeStruct((1, 128, 512), BF16), jax.ShapeDtypeStruct((24, 512), F32)),
        in_specs=[hbm] * 10,
        out_specs=(vmem, vmem),
        scratch_shapes=[
            v((128, 256), BF16),
            v((6, 1, 128), jnp.int32),
            v((1, 1, 8, 32), jnp.int32),
            pltpu.SMEM((1, 32), jnp.int32),
            pltpu.SMEM((1, 2, 4), jnp.int32),
            v((1, 512), F32),
            v((2, 128, 128), F32),
            v((32, 1, 128), jnp.int32),
            v((32, 1, 128), jnp.int32),
            v((48, 8, 256), BF16),
            v((32, 8, 256), BF16),
            v((128, 256), BF16),
            v((768, 384), BF16),
            v((6, 128, 256), BF16),
            v((3, 8, 128), BF16),
            v((2, 8, 128), BF16),
            v((2, 2, 8, 128), BF16),
            v((16, 3, 2, NZ, 8, 128), BF16),
            v((16, 2, NZ, 8, 128), BF16),
            v((128, 512), F32),
            v((2, 128, 512), BF16),
            v((256, 1152), BF16),
            v((8, 128), F32),
            v((32, 8, 128), BF16),
            v((2, 32, 256), BF16),
            v((2, 8, 768), BF16),
            v((6, 256, 128), BF16),
            v((6, 128, 128), F32),
            v((6, 1, 256), F32),
            v((6, 1, 256), F32),
            v((2, 128, 512), BF16),
            v((2, 384, 128), BF16),
            v((2, 384, 128), BF16),
            v((4, 8, 2, 3, 8, 128), BF16),
            v((3, 8, 2, 3, 8, 128), BF16),
            v((8, 2, 3, 8, 128), BF16),
            v((NZ, 3, 8, 128), BF16),
            v((16, 3, 8, 128), BF16),
            v((256, 256), BF16),
            v((512, 512), BF16),
            v((768, 768), BF16),
            pltpu.SemaphoreType.DMA((20,)),
            pltpu.SemaphoreType.DMA((43,)),
            pltpu.SemaphoreType.DMA((59,)),
        ],
        compiler_params=pltpu.CompilerParams(
            collective_id=0, has_side_effects=True, vmem_limit_bytes=VMEM
        ),
    )(
        *(
            pltpu.with_memory_space_constraint(array, pltpu.HBM)
            for array in (
                feats, near_map.transpose(2, 0, 1), wanted.swapaxes(2, 3), counts, choice, conv, gain.reshape(1, -1), inw, outw, cot
            )
        )
    )


def solution(mesh):
    space = ("z", "c")
    dp = ("y", "x")
    torus = Mesh(mesh.devices.reshape(4, 4, 16, 2), dp + space)
    return jax.shard_map(
        shards,
        mesh=torus,
        in_specs=(
            P(dp, space, None),
            P(dp, space, None),
            P(dp, space, None, None),
            P(dp, None),
            P(dp, space, None),
            P(None, space, None),
            P(),
            P(space, None),
            P(space, None),
            P(dp, space, None),
        ),
        out_specs=(P(dp, space, None), P(space, None)),
        check_vma=False,
    )
```

```python
import jax
import jax.numpy as jnp
from jax import lax
from jax.experimental import pallas as pl
from jax.experimental.pallas import tpu as pltpu
from jax.sharding import Mesh
from jax.sharding import PartitionSpec as P

MESH = pl.DeviceIdType.MESH
F32 = jnp.float32
BF16 = jnp.bfloat16
NZ = 16
VMEM = 48 * 1024 * 1024
CHUNKS = {0: (0, 2, 0, 8, 0), 1: (0, 2, 8, 16, 0), 2: (0, 2, 0, 8, 1), 3: (0, 2, 8, 16, 1), 7: (2, 3, 0, 16, 0)}
RELAYED = (7,)
SPLIT = {4: (0, 8, 0), 5: (8, 16, 0), 6: (0, 8, 1), 8: (8, 16, 1)}
LAST = 8


def iota(shape, dim):
    return lax.broadcasted_iota(jnp.int32, shape, dim)


def one_hot(flags):
    return jnp.where(flags, 1.0, 0.0).astype(BF16)


def ordering(parts, z):
    n = 256 * parts
    col = iota((1, n), 1)
    slot = (col >> 3) & 15
    chip = (z + NZ + jnp.where((slot & 1) == 1, (slot + 1) >> 1, -(slot >> 1))) & 15
    natural = chip * (16 * parts) + ((col >> 7) & 1) * (8 * parts) + (col >> 8) * 8 + (col & 7)
    return one_hot(iota((n, n), 0) == natural)


def dot(a, b):
    return jnp.dot(a, b, preferred_element_type=F32)


def dot_t(a, b):
    return lax.dot_general(a, b, (((1,), (1,)), ((), ())), preferred_element_type=F32)


def turned_dot(a, b):
    return lax.dot_general(a, b, (((0,), (0,)), ((), ())), preferred_element_type=F32)


def drain(ref, sem):
    pltpu.make_async_copy(ref, ref, sem).wait()


def kernel(
    feats_h, near_h, wanted_h, counts_h, choice_h, conv_h, gain_h, inw_h, outw_h, cot_h,
    layer, grad,
    feats, near_map, wanted, counts, choice, gain, turned,
    asked, asks, table, answers, own_feats, taps_hot, taps, staged, staged_far, staged_in, held, split_in,
    hidden, normed_all, qkv, tall, shorts, chosen_hot, picked, split_q, near_mix, near_top, near_sum, cot, att, att_all, terms, across, summed, along, final,
    order_taps, order_in, order_out,
    local_sem, send_sem, recv_sem,
):
    y, x, z, c = (lax.axis_index(n) for n in ("y", "x", "z", "c"))
    other = 1 - c
    me = z * 2 + c
    plane = y * 4 + x
    a = (1 - c) * x + c * y
    b = (1 - c) * y + c * x
    piece = b * 4 + a
    b_far = lax.rem(b + 2, 4)
    piece_far = b_far * 4 + a
    core_pieces = ((y * 4 + x, lax.rem(y + 2, 4) * 4 + x), (x * 4 + y, lax.rem(x + 2, 4) * 4 + y))

    def z_of(slot):
        return lax.rem(z + NZ - (2 * lax.rem(slot, 2) - 1) * ((slot + 1) // 2), NZ)

    def a_peer(d):
        t = lax.rem(a + d, 4)
        return t, {"x": (1 - c) * t + c * x, "y": (1 - c) * y + c * t}

    def b_peer(d):
        t = lax.rem(b + d, 4)
        return t, {"x": (1 - c) * x + c * t, "y": (1 - c) * t + c * y}

    def plane_peer(k):
        t = lax.rem(plane + k, 16)
        return {"y": t // 4, "x": lax.rem(t, 4)}

    def send(src, dst, s, r, where):
        pltpu.make_async_remote_copy(
            src_ref=src, dst_ref=dst, send_sem=send_sem.at[s], recv_sem=recv_sem.at[r],
            device_id=where, device_id_type=MESH,
        ).start()

    def fetch(src, dst, k):
        copy = pltpu.make_async_copy(src, dst, local_sem.at[k])
        copy.start()
        return copy

    first = [
        fetch(wanted_h, wanted, 6),
        fetch(near_h, near_map, 7),
        fetch(feats_h.at[0], feats, 8),
    ]

    barrier = pltpu.get_barrier_semaphore()

    def hail(where):
        pl.semaphore_signal(barrier, inc=1, device_id=where, device_id_type=MESH)

    def hail_z(i, _):
        hail({"z": z_of(i), "c": 0})
        hail({"z": z_of(i), "c": 1})
        return 0

    lax.fori_loop(1, NZ, lambda i, _: hail_z(NZ - i, _), 0)
    lax.fori_loop(1, 16, lambda k, _: (hail(plane_peer(k)), 0)[1], 0)
    hail({"c": other})

    lanes = pl.ds(pl.multiple_of(a * 128, 128), 128)
    later = [
        fetch(counts_h, counts, 9),
        fetch(choice_h, choice, 10),
        fetch(gain_h, gain, 11),
    ]
    copies = [
        fetch(cot_h.at[0], cot.at[c], 0),
        fetch(conv_h.at[2 * b, :, lanes], staged.at[0], 1),
        fetch(conv_h.at[2 * b_far, :, lanes], staged_far.at[0], 12),
        fetch(outw_h.at[pl.ds(pl.multiple_of(lax.rem(b, 3) * 8, 8), 8), lanes], staged.at[2], 5),
        *(
            fetch(
                inw_h.at[
                    pl.ds(pl.multiple_of(lax.rem(p, 2) * 8, 8), 8),
                    pl.ds(pl.multiple_of((p // 6 * 6 + 3 * h + lax.rem(p // 2, 3)) * 128, 128), 128),
                ],
                staged_in.at[h, far], 16 + 2 * h + far,
            )
            for h in range(2) for far, p in enumerate(core_pieces[h])
        ),
    ]

    for k, (at, to) in enumerate(((b, staged), (b_far, staged_far))):

        @pl.when(at < 3)
        def _(k=k, at=at, to=to):
            fetch(conv_h.at[2 * at + 1, :, lanes], to.at[1], 2 + 11 * k)

        @pl.when(at == 3)
        def _(k=k, to=to):
            half_rows = pl.ds(pl.multiple_of(lax.rem(a, 2) * 8, 8), 8)
            fetch(inw_h.at[half_rows, pl.ds(pl.multiple_of((14 + 3 * (a // 2)) * 128, 128), 128)], to.at[1], 2 + 11 * k)

    turned[...] = jnp.zeros_like(turned)
    for copy in first:
        copy.wait()
    turned[0, 0:8, 0:32] = wanted[0, 0].astype(F32)
    for k in range(6):
        turned[1, k : k + 1, :] = near_map[k].astype(F32)
    lists = turned[0].T[0:32].astype(jnp.int32)
    slots = jnp.zeros((32, 128), jnp.int32)
    for k in range(8):
        slots = slots + jnp.where(lists[:, k : k + 1] == iota((32, 128), 1), 1 << k, 0)
    for p in range(32):
        asks[p] = slots[p : p + 1, :]
    asked[me] = asks[me]
    rows = turned[1].T
    for k in range(6):
        taps_hot[128 * k : 128 * (k + 1), :] = one_hot(rows[:, k : k + 1].astype(jnp.int32) == iota((128, 384), 1))
    order_taps[...] = ordering(1, z)
    ordered = dot(feats[...], order_taps[...]).astype(BF16)
    own_feats[...] = ordered
    table[0:16] = ordered.reshape(16, 8, 256)
    for copy in copies:
        copy.wait()
    drain(staged.at[1], local_sem.at[2])
    drain(staged_far.at[1], local_sem.at[13])
    held[piece, :, c, 0] = staged[...]
    held[piece_far, 0:2, c, 0] = staged_far[...]
    split_in[piece, c, 0] = staged_in[c, 0]
    split_in[piece_far, c, 0] = staged_in[c, 1]
    with jax.named_scope("w_barrier"):
        pl.semaphore_wait(barrier, 46)

    def far_first(body):
        lax.fori_loop(1, NZ, lambda i, _: (body(NZ - i), 0)[1], 0)

    def ask(slot):
        t = z_of(slot)
        for core in range(2):
            send(asks.at[t * 2 + core], asked.at[me], 0, 0, {"z": t, "c": core})

    def spread(n):
        lo, hi, s0, s1, far = CHUNKS[n]

        def one(slot, _):
            source, p = (staged_far.at[lo:hi], piece_far) if far else (staged.at[lo:hi], piece)
            send(source, held.at[p, lo:hi, c, slot], 5 + n, 7 + n, {"z": z_of(slot)})
            return 0

        lax.fori_loop(max(s0, 1), s1, one, 0)

    def along_z(n):
        return (43, 59) if n == LAST else (5 + n, 7 + n)

    def along_axis(n):
        return (44, 60) if n == LAST else (13 + n, 15 + n)

    def spread_in(n):
        s0, s1, far = SPLIT[n]

        def one(slot, _):
            for h in range(2):
                send(staged_in.at[h, far], split_in.at[core_pieces[h][far], c, slot], *along_z(n), {"z": z_of(slot), "c": h})
            return 0

        if s0 == 0:
            p = (1 - other) * core_pieces[0][far] + other * core_pieces[1][far]
            send(staged_in.at[other, far], split_in.at[p, c, 0], *along_z(n), {"c": other})
        lax.fori_loop(max(s0, 1), s1, one, 0)

    def arrivals(n):
        return split_in.at[0, 0, 0 : 15 if SPLIT[n][0] == 0 else 16]

    far_first(ask)
    send(asks.at[z * 2 + other], asked.at[me], 0, 0, {"c": other})
    for n in range(4):
        spread(n)
    spread_in(4)
    spread_in(5)
    send(cot.at[c], cot.at[c], 1, 1, {"c": other})
    for copy in later:
        copy.wait()
    m32 = iota((32, 1), 0)
    target = jnp.zeros((32, 1), jnp.int32)
    for e in range(8):
        block = choice[0, e // 4, e % 4]
        target = jnp.where((m32 & 7) == e, (block // 2) * 8 + lax.rem(block, 2), target)
    chosen_hot[c] = one_hot(target + 2 * (m32 >> 3) == iota((32, 256), 1))
    order_in[...] = ordering(2, z)
    order_out[...] = ordering(3, z)

    def part(n, p, count, from_slot=None, to_slot=None):
        lo, hi, s0, s1, _ = CHUNKS[n]
        return held.at[pl.ds(p, count), lo:hi, c, s0 if from_slot is None else from_slot : s1 if to_slot is None else to_slot]

    def cross(n, p, count):
        some = part(n, p, count)
        send(some, some, 29 + n, 47 + n, {"c": other})

    def along_a(n):
        lo, hi, s0, s1, far = CHUNKS[n]
        with jax.named_scope(f"w_z{n}"):
            drain(held.at[0, lo:hi, 0, max(s0, 1) : s1], recv_sem.at[7 + n])
        some = part(n, piece_far if far else piece, 1)
        for d in (2, 1, 3):
            send(some, some, 13 + n, 15 + n, a_peer(d)[1])

    def along_b(n):
        lo, hi, s0, s1, far = CHUNKS[n]
        with jax.named_scope(f"w_a{n}"):
            drain(held.at[0:3, lo:hi, 0, s0:s1], recv_sem.at[15 + n])
        if not far:
            for k, d in enumerate((1, 3)):
                send(part(n, b * 4, 4), part(n, b * 4, 4), 21 + n, 23 + 8 * k + n, b_peer(d)[1])
        cross(n, (b_far if far else b) * 4, 4)

    def relay(n):
        lo, hi, s0, s1, _ = CHUNKS[n]
        middle = (s0 + s1) // 2
        for k, d, low, high in ((0, 1, s0, middle), (1, 3, middle, s1)):
            source = lax.rem(b + 4 - d, 4) * 4
            with jax.named_scope(f"w_b{n}"):
                drain(part(n, source, 4), recv_sem.at[23 + 8 * k + n])
            if n in RELAYED:
                send(part(n, source, 4, low, high), part(n, source, 4, low, high), 21 + n, 39 + n, b_peer(d)[1])
            cross(n, source, 4)

    def last(n):
        with jax.named_scope(f"w_f{n}"):
            drain(part(n, b_far * 4, 4), recv_sem.at[39 + n])
        cross(n, b_far * 4, 4)

    def part_in(n, p, count):
        s0, s1, _ = SPLIT[n]
        return split_in.at[pl.ds(p, count), :, s0:s1]

    def split_a(n):
        with jax.named_scope(f"w_z{n}"):
            drain(arrivals(n), recv_sem.at[along_z(n)[1]])
        some = part_in(n, piece_far if SPLIT[n][2] else piece, 1)
        for d in (2, 1, 3):
            send(some, some, *along_axis(n), a_peer(d)[1])

    def split_b(n):
        with jax.named_scope(f"w_a{n}"):
            drain(part_in(n, 0, 3), recv_sem.at[along_axis(n)[1]])
        if not SPLIT[n][2]:
            for k, d in enumerate((1, 3)):
                send(part_in(n, b * 4, 4), part_in(n, b * 4, 4), 21 + n, 23 + 8 * k + n, b_peer(d)[1])

    def split_end(n):
        for k, d in ((0, 1), (1, 3)):
            with jax.named_scope(f"w_b{n}"):
                drain(part_in(n, lax.rem(b + 4 - d, 4) * 4, 4), recv_sem.at[23 + 8 * k + n])

    def crossings(n):
        return 16 if n in RELAYED else 4 if CHUNKS[n][4] else 12

    def crossed(n):
        lo, hi, s0, s1, _ = CHUNKS[n]
        with jax.named_scope(f"w_c{n}"):
            drain(held.at[0 : crossings(n), lo:hi, 0, s0:s1], recv_sem.at[47 + n])

    send(chosen_hot.at[c], chosen_hot.at[c], 4, 4, {"c": other})
    along_a(0)

    with jax.named_scope("w_ask"):
        drain(asked.at[0:31], recv_sem.at[0])
    wants = jnp.broadcast_to(asked[...], (32, 8, 128))
    wants = one_hot(((wants >> iota((32, 8, 128), 1)) & 1) == 1).reshape(256, 128)
    picked_rows = dot(wants, feats[...]).astype(BF16)
    answers[...] = picked_rows.reshape(32, 8, 256)
    table[16 + me] = answers[me]

    def answer(slot):
        t = z_of(slot)
        for core in range(2):
            send(answers.at[t * 2 + core], table.at[16 + me], 2, 2, {"z": t, "c": core})

    far_first(answer)
    send(answers.at[z * 2 + other], table.at[16 + me], 2, 2, {"c": other})
    spread_in(8)
    spread_in(6)
    spread(7)

    along_a(1)
    along_b(0)
    along_a(2)
    along_a(3)
    along_b(1)
    relay(0)
    split_a(4)
    split_a(5)
    along_b(2)
    along_b(3)
    relay(1)
    with jax.named_scope("w_rows"):
        drain(table.at[0:31], recv_sem.at[2])
    fetched = table[16:48].reshape(256, 256)
    table[16:48] = dot(fetched, order_taps[...]).astype(BF16).reshape(32, 8, 256)
    for k in range(3):
        got = dot(taps_hot[256 * k : 256 * (k + 1), :], table[...].reshape(384, 256))
        taps[2 * k : 2 * k + 2] = got.astype(BF16).reshape(2, 128, 256)
    split_b(4)
    for n in range(4):
        crossed(n)
    split_b(5)

    def unit(p, u):
        return held[p, u].reshape(256, 128)

    count = counts[0, me]
    alive = jnp.where(iota((128, 128), 0) < count, 1.0, 0.0)
    alive_wide = jnp.concatenate([alive, alive], axis=1)
    for t in range(0, 4, 2):
        total = jnp.zeros((128, 256), F32)
        for k in range(7):
            p, u = (k // 2) * 4 + t, k % 2
            tap = own_feats[...] if k == 0 else taps[k - 1]
            total = total + dot(tap, jnp.concatenate([unit(p, u), unit(p + 1, u)], axis=1))
        hidden[:, 128 * t : 128 * (t + 2)] = total * alive_wide
    h = hidden[...]
    power = jnp.mean(h * h, axis=-1, keepdims=True)
    normed = (h * lax.rsqrt(power + 1e-06) * gain[...]).astype(BF16)

    token = iota((8, 128), 1)
    block_mask = one_hot(((token >> 6) == iota((8, 128), 0)) & (token < count))
    number = jnp.clip(count - 64 * iota((8, 1), 0), 0, 64)
    means = dot(block_mask, normed) / jnp.maximum(number, 1).astype(F32)
    for j in range(4):
        tall[2 * j : 2 * j + 2, :] = means[0:2, 128 * j : 128 * (j + 1)]
    shorts[me] = tall[...].astype(BF16)

    def tell(slot):
        for core in range(2):
            send(shorts.at[me], shorts.at[me], 3, 3, {"z": z_of(slot), "c": core})

    far_first(tell)
    send(shorts.at[me], shorts.at[me], 3, 3, {"c": other})

    normed_all[c] = dot(normed, order_in[...]).astype(BF16)
    send(normed_all.at[c], normed_all.at[c], 38, 6, {"c": other})
    split_a(6)
    split_a(8)
    split_end(4)
    with jax.named_scope("w_norm"):
        drain(normed_all.at[0], recv_sem.at[6])
    split_end(5)
    split_b(6)
    split_b(8)

    def unit_in(tile, i):
        if tile < 8:
            return split_in[2 * tile + i].reshape(256, 128)
        return held[12 + 2 * c + i, 1].reshape(256, 128)

    def project(rows, tiles):
        upper = jnp.concatenate([unit_in(t, 0) for t in tiles], axis=1)
        lower = jnp.concatenate([unit_in(t, 1) for t in tiles], axis=1)
        return dot(rows[:, :256], upper) + dot(rows[:, 256:], lower)

    tokens = normed_all[...].reshape(256, 512)
    for tiles in ((0, 1), (2, 3), (4, 5), (6, 7), (8,)):
        qkv[:, 128 * tiles[0] : 128 * (tiles[-1] + 1)] = project(tokens, tiles).astype(BF16)

    half = iota((128, 128), 1) < 64
    key = iota((128, 256), 0)
    same_block = (key >> 6) == ((iota((128, 256), 1) & 127) >> 6)
    for core in range(2):
        near_ok = same_block & (key < counts[0, 2 * z + core])
        rows = slice(128 * core, 128 * (core + 1))
        for j in range(3):
            at = 3 * core + j
            q = qkv[rows, 128 * j : 128 * (j + 1)] * jnp.asarray(0.125, BF16)
            none = jnp.zeros_like(q)
            q = jnp.concatenate([jnp.where(half, q, none), jnp.where(half, none, q)], axis=0)
            split_q[at] = q
            near = jnp.where(near_ok, dot_t(qkv[rows, 384 + 128 * j : 384 + 128 * (j + 1)], q), -1e30)
            top = jnp.max(near, axis=0, keepdims=True)
            near = jnp.exp(near - top)
            near_top[at] = top
            near_sum[at] = jnp.sum(near, axis=0, keepdims=True)
            mixed = turned_dot(qkv[rows, 768 + 128 * j : 768 + 128 * (j + 1)], near.astype(BF16))
            near_mix[at, 0:64] = mixed[0:64, 0:128]
            near_mix[at, 64:128] = mixed[64:128, 128:256]
    along_a(7)
    drain(chosen_hot.at[0], recv_sem.at[4])
    drain(cot.at[0], recv_sem.at[1])

    with jax.named_scope("w_short"):
        drain(shorts.at[0:31], recv_sem.at[3])
    chosen = dot(chosen_hot[...].reshape(64, 256), shorts[...].reshape(256, 128))
    chosen = jnp.concatenate(
        [jnp.concatenate([chosen[32 * k + 8 * j : 32 * k + 8 * j + 8] for j in range(4)], axis=1) for k in range(2)], axis=0
    ).astype(BF16)
    chosen = dot(chosen, order_in[...]).astype(BF16)
    for tiles in ((3, 4), (5, 6), (7, 8)):
        got = project(chosen, tiles)
        for k in range(2):
            picked[k, :, 128 * (tiles[0] - 3) : 128 * (tiles[0] - 1)] = got[8 * k : 8 * k + 8].astype(BF16)
    far_ok = (iota((8, 256), 0) >> 2) == ((iota((8, 256), 1) & 127) >> 6)
    for j in range(3):
        for core in range(2):
            at = 3 * core + j
            alive_row = jnp.where(iota((1, 128), 1) < counts[0, 2 * z + core], 1.0, 0.0)
            far = jnp.where(far_ok, dot_t(picked[core, :, 128 * j : 128 * (j + 1)], split_q[at]), -1e30)
            top = jnp.maximum(near_top[at], jnp.max(far, axis=0, keepdims=True))
            keep, far = jnp.exp(near_top[at] - top), jnp.exp(far - top)
            scale = 1.0 / (near_sum[at] * keep + jnp.sum(far, axis=0, keepdims=True))
            mixed = turned_dot(picked[core, :, 384 + 128 * j : 384 + 128 * (j + 1)], far.astype(BF16))
            for k in range(2):
                rows, cols = slice(64 * k, 64 * (k + 1)), slice(128 * k, 128 * (k + 1))
                both = near_mix[at, rows] * keep[:, cols] + mixed[rows, cols]
                att[core, 128 * j + 64 * k : 128 * j + 64 * (k + 1)] = (both * (scale[:, cols] * alive_row)).astype(BF16)
        if j == 0:
            continue
        g = j - 1
        rows = slice(192 * g, 192 * (g + 1))
        both = jnp.concatenate([att[0, rows], att[1, rows]], axis=1)
        for t in range(0, 4, 2):
            got = dot(both, cot[:, :, 128 * t : 128 * (t + 2)].reshape(256, 256))
            for k in range(2):
                terms[t + k, 4 * g : 4 * g + 4] = got[:, 128 * k : 128 * (k + 1)].astype(BF16).reshape(4, 2, 3, 8, 128)
        for d in (2, 1, 3):
            t, where = a_peer(d)
            send(terms.at[t, 4 * g : 4 * g + 4], across.at[d - 1, 4 * g : 4 * g + 4], 39 + g, 55 + g, where)
    att_all[c] = att[c]
    send(att.at[other], att_all.at[c], 37, 5, {"c": other})

    for g in range(2):
        rows = slice(4 * g, 4 * (g + 1))
        with jax.named_scope(f"w_across{g}"):
            drain(across.at[:, rows], recv_sem.at[55 + g])
        total = terms[a, rows].astype(F32)
        for d in range(3):
            total = total + across[d, rows].astype(F32)
        summed[rows] = total.astype(BF16)

        def reduce_z(k, _):
            for core in range(2):

                @pl.when((8 * c + k) * 2 + core != me)
                def _():
                    send(summed.at[k, core], along.at[z], 41, 57, {"z": 8 * c + k, "c": core})

            return 0

        lax.fori_loop(4 * g, 4 * (g + 1), reduce_z, 0)
    along_b(7)
    mine = z // 8 == c

    @pl.when(mine)
    def _():
        along[z] = summed[z - 8 * c, c]

    relay(7)
    with jax.named_scope("w_along"):

        @pl.when(mine)
        def _():
            drain(along.at[0:15], recv_sem.at[57])

        @pl.when(jnp.logical_not(mine))
        def _():
            drain(along, recv_sem.at[57])

    total = along[0].astype(F32)
    for k in range(1, NZ):
        total = total + along[k].astype(F32)
    sender = z // 8
    summed_piece = (1 - sender) * core_pieces[0][0] + sender * core_pieces[1][0]
    final[summed_piece] = total.astype(BF16)

    for dy, dx in sorted(((dy, dx) for dy in range(4) for dx in range(4)), key=lambda d: -(d[0] * (4 - d[0]) + d[1] * (4 - d[1]))):
        if (dy, dx) != (0, 0):
            where = {"y": lax.rem(y + dy, 4), "x": lax.rem(x + dx, 4)}
            send(final.at[summed_piece], final.at[summed_piece], 42, 58, where)
    last(7)
    crossed(7)
    drain(att_all.at[0], recv_sem.at[5])
    attended = turned_dot(att_all[...].reshape(768, 128), order_out[...]).astype(BF16)
    for t in range(0, 4, 2):
        total = hidden[:, 128 * t : 128 * (t + 2)]
        for i in range(3):
            w = jnp.concatenate([unit(4 * i + t, 2), unit(4 * i + t + 1, 2)], axis=1)
            total = total + dot(attended[:, 256 * i : 256 * (i + 1)], w)
        layer[0, :, 128 * t : 128 * (t + 2)] = total.astype(BF16)

    drain(asked.at[0:31], send_sem.at[0])
    drain(cot.at[0], send_sem.at[1])
    drain(table.at[0:31], send_sem.at[2])
    drain(shorts.at[0:31], send_sem.at[3])
    for n, (lo, hi, s0, s1, far) in CHUNKS.items():
        drain(held.at[0, lo:hi, 0, max(s0, 1) : s1], send_sem.at[5 + n])
        drain(held.at[0:3, lo:hi, 0, s0:s1], send_sem.at[13 + n])
        if not far:
            drain(held.at[0 : 12 if n in RELAYED else 8, lo:hi, 0, s0:s1], send_sem.at[21 + n])
        drain(held.at[0 : crossings(n), lo:hi, 0, s0:s1], send_sem.at[29 + n])
    for n, (s0, s1, far) in SPLIT.items():
        drain(arrivals(n), send_sem.at[along_z(n)[0]])
        drain(part_in(n, 0, 3), send_sem.at[along_axis(n)[0]])
        if not far:
            drain(part_in(n, 0, 8), send_sem.at[21 + n])
    drain(chosen_hot.at[0], send_sem.at[4])
    drain(normed_all.at[0], send_sem.at[38])
    drain(att_all.at[0], send_sem.at[37])
    for g in range(2):
        drain(across.at[:, 4 * g : 4 * (g + 1)], send_sem.at[39 + g])

    @pl.when(mine)
    def _():
        drain(along.at[0:15], send_sem.at[41])

    @pl.when(jnp.logical_not(mine))
    def _():
        drain(along, send_sem.at[41])

    with jax.named_scope("w_final"):
        drain(final.at[0:15], recv_sem.at[58])
    factor = (16 * 4096) ** -0.5
    for t in range(4):
        total = final[t].astype(F32)
        for k in range(1, 4):
            total = total + final[4 * k + t].astype(F32)
        grad[:, 128 * t : 128 * (t + 1)] = total.reshape(24, 128) * factor

    drain(final.at[0:15], send_sem.at[42])


def shards(feats, near_map, wanted, counts, choice, conv, gain, inw, outw, cot):
    vmem = pl.BlockSpec(memory_space=pltpu.VMEM)
    hbm = pl.BlockSpec(memory_space=pltpu.HBM)
    v = pltpu.VMEM
    return pl.pallas_call(
        kernel,
        name="layer",
        out_shape=(jax.ShapeDtypeStruct((1, 128, 512), BF16), jax.ShapeDtypeStruct((24, 512), F32)),
        in_specs=[hbm] * 10,
        out_specs=(vmem, vmem),
        scratch_shapes=[
            v((128, 256), BF16),
            v((6, 1, 128), jnp.int32),
            v((1, 1, 8, 32), jnp.int32),
            pltpu.SMEM((1, 32), jnp.int32),
            pltpu.SMEM((1, 2, 4), jnp.int32),
            v((1, 512), F32),
            v((2, 128, 128), F32),
            v((32, 1, 128), jnp.int32),
            v((32, 1, 128), jnp.int32),
            v((48, 8, 256), BF16),
            v((32, 8, 256), BF16),
            v((128, 256), BF16),
            v((768, 384), BF16),
            v((6, 128, 256), BF16),
            v((3, 8, 128), BF16),
            v((2, 8, 128), BF16),
            v((2, 2, 8, 128), BF16),
            v((16, 3, 2, NZ, 8, 128), BF16),
            v((16, 2, NZ, 8, 128), BF16),
            v((128, 512), F32),
            v((2, 128, 512), BF16),
            v((256, 1152), BF16),
            v((8, 128), F32),
            v((32, 8, 128), BF16),
            v((2, 32, 256), BF16),
            v((2, 8, 768), BF16),
            v((6, 256, 128), BF16),
            v((6, 128, 128), F32),
            v((6, 1, 256), F32),
            v((6, 1, 256), F32),
            v((2, 128, 512), BF16),
            v((2, 384, 128), BF16),
            v((2, 384, 128), BF16),
            v((4, 8, 2, 3, 8, 128), BF16),
            v((3, 8, 2, 3, 8, 128), BF16),
            v((8, 2, 3, 8, 128), BF16),
            v((NZ, 3, 8, 128), BF16),
            v((16, 3, 8, 128), BF16),
            v((256, 256), BF16),
            v((512, 512), BF16),
            v((768, 768), BF16),
            pltpu.SemaphoreType.DMA((20,)),
            pltpu.SemaphoreType.DMA((45,)),
            pltpu.SemaphoreType.DMA((61,)),
        ],
        compiler_params=pltpu.CompilerParams(
            collective_id=0, has_side_effects=True, vmem_limit_bytes=VMEM
        ),
    )(
        *(
            pltpu.with_memory_space_constraint(array, pltpu.HBM)
            for array in (
                feats, near_map.transpose(2, 0, 1), wanted.swapaxes(2, 3), counts, choice, conv, gain.reshape(1, -1), inw, outw, cot
            )
        )
    )


def solution(mesh):
    space = ("z", "c")
    dp = ("y", "x")
    torus = Mesh(mesh.devices.reshape(4, 4, 16, 2), dp + space)
    return jax.shard_map(
        shards,
        mesh=torus,
        in_specs=(
            P(dp, space, None),
            P(dp, space, None),
            P(dp, space, None, None),
            P(dp, None),
            P(dp, space, None),
            P(None, space, None),
            P(),
            P(space, None),
            P(space, None),
            P(dp, space, None),
        ),
        out_specs=(P(dp, space, None), P(space, None)),
        check_vma=False,
    )
```

```python
import jax
import jax.numpy as jnp
from jax import lax
from jax.experimental import pallas as pl
from jax.experimental.pallas import tpu as pltpu
from jax.sharding import Mesh
from jax.sharding import PartitionSpec as P

MESH = pl.DeviceIdType.MESH
F32 = jnp.float32
BF16 = jnp.bfloat16
NZ = 16
VMEM = 48 * 1024 * 1024
CHUNKS = {0: (0, 2, 0, 8, 0), 1: (0, 2, 8, 16, 0), 2: (0, 2, 0, 8, 1), 3: (0, 2, 8, 16, 1), 7: (2, 3, 0, 16, 0)}
RELAYED = (7,)
SPLIT = {4: (0, 8, 0), 5: (8, 16, 0), 6: (0, 8, 1), 8: (8, 16, 1)}
LAST = 8


def iota(shape, dim):
    return lax.broadcasted_iota(jnp.int32, shape, dim)


def one_hot(flags):
    return jnp.where(flags, 1.0, 0.0).astype(BF16)


def ordering(parts, z):
    n = 256 * parts
    col = iota((1, n), 1)
    slot = (col >> 3) & 15
    chip = (z + NZ + jnp.where((slot & 1) == 1, (slot + 1) >> 1, -(slot >> 1))) & 15
    natural = chip * (16 * parts) + ((col >> 7) & 1) * (8 * parts) + (col >> 8) * 8 + (col & 7)
    return one_hot(iota((n, n), 0) == natural)


def dot(a, b):
    return jnp.dot(a, b, preferred_element_type=F32)


def dot_t(a, b):
    return lax.dot_general(a, b, (((1,), (1,)), ((), ())), preferred_element_type=F32)


def turned_dot(a, b):
    return lax.dot_general(a, b, (((0,), (0,)), ((), ())), preferred_element_type=F32)


def drain(ref, sem):
    pltpu.make_async_copy(ref, ref, sem).wait()


def kernel(
    feats_h, near_h, wanted_h, counts_h, choice_h, conv_h, gain_h, inw_h, outw_h, cot_h,
    layer, grad,
    feats, near_map, wanted, counts, choice, gain, turned,
    asked, asks, table, answers, own_feats, taps_hot, taps, staged, staged_far, staged_in, held, split_in,
    hidden, normed_all, qkv, tall, shorts, chosen_hot, picked, split_q, near_mix, near_top, near_sum, cot, att, att_all, terms, across, summed, along, final,
    order_taps, order_in, order_out,
    local_sem, send_sem, recv_sem,
):
    y, x, z, c = (lax.axis_index(n) for n in ("y", "x", "z", "c"))
    other = 1 - c
    me = z * 2 + c
    plane = y * 4 + x
    a = (1 - c) * x + c * y
    b = (1 - c) * y + c * x
    piece = b * 4 + a
    b_far = lax.rem(b + 2, 4)
    piece_far = b_far * 4 + a
    core_pieces = ((y * 4 + x, lax.rem(y + 2, 4) * 4 + x), (x * 4 + y, lax.rem(x + 2, 4) * 4 + y))

    def z_of(slot):
        return lax.rem(z + NZ - (2 * lax.rem(slot, 2) - 1) * ((slot + 1) // 2), NZ)

    def a_peer(d):
        t = lax.rem(a + d, 4)
        return t, {"x": (1 - c) * t + c * x, "y": (1 - c) * y + c * t}

    def b_peer(d):
        t = lax.rem(b + d, 4)
        return t, {"x": (1 - c) * x + c * t, "y": (1 - c) * t + c * y}

    def plane_peer(k):
        t = lax.rem(plane + k, 16)
        return {"y": t // 4, "x": lax.rem(t, 4)}

    def send(src, dst, s, r, where):
        pltpu.make_async_remote_copy(
            src_ref=src, dst_ref=dst, send_sem=send_sem.at[s], recv_sem=recv_sem.at[r],
            device_id=where, device_id_type=MESH,
        ).start()

    def fetch(src, dst, k):
        copy = pltpu.make_async_copy(src, dst, local_sem.at[k])
        copy.start()
        return copy

    first = [
        fetch(wanted_h, wanted, 6),
        fetch(near_h, near_map, 7),
        fetch(feats_h.at[0], feats, 8),
    ]

    barrier = pltpu.get_barrier_semaphore()

    def hail(where):
        pl.semaphore_signal(barrier, inc=1, device_id=where, device_id_type=MESH)

    def hail_z(i, _):
        hail({"z": z_of(i), "c": 0})
        hail({"z": z_of(i), "c": 1})
        return 0

    lax.fori_loop(1, NZ, lambda i, _: hail_z(NZ - i, _), 0)
    lax.fori_loop(1, 16, lambda k, _: (hail(plane_peer(k)), 0)[1], 0)
    hail({"c": other})

    lanes = pl.ds(pl.multiple_of(a * 128, 128), 128)
    later = [
        fetch(counts_h, counts, 9),
        fetch(choice_h, choice, 10),
        fetch(gain_h, gain, 11),
    ]
    copies = [
        fetch(cot_h.at[0], cot.at[c], 0),
        fetch(conv_h.at[2 * b, :, lanes], staged.at[0], 1),
        fetch(conv_h.at[2 * b_far, :, lanes], staged_far.at[0], 12),
        fetch(outw_h.at[pl.ds(pl.multiple_of(lax.rem(b, 3) * 8, 8), 8), lanes], staged.at[2], 5),
        *(
            fetch(
                inw_h.at[
                    pl.ds(pl.multiple_of(lax.rem(p, 2) * 8, 8), 8),
                    pl.ds(pl.multiple_of((p // 6 * 6 + 3 * h + lax.rem(p // 2, 3)) * 128, 128), 128),
                ],
                staged_in.at[h, far], 16 + 2 * h + far,
            )
            for h in range(2) for far, p in enumerate(core_pieces[h])
        ),
    ]

    for k, (at, to) in enumerate(((b, staged), (b_far, staged_far))):

        @pl.when(at < 3)
        def _(k=k, at=at, to=to):
            fetch(conv_h.at[2 * at + 1, :, lanes], to.at[1], 2 + 11 * k)

        @pl.when(at == 3)
        def _(k=k, to=to):
            half_rows = pl.ds(pl.multiple_of(lax.rem(a, 2) * 8, 8), 8)
            fetch(inw_h.at[half_rows, pl.ds(pl.multiple_of((14 + 3 * (a // 2)) * 128, 128), 128)], to.at[1], 2 + 11 * k)

    turned[...] = jnp.zeros_like(turned)
    for copy in first:
        copy.wait()
    turned[0, 0:8, 0:32] = wanted[0, 0].astype(F32)
    for k in range(6):
        turned[1, k : k + 1, :] = near_map[k].astype(F32)
    lists = turned[0].T[0:32].astype(jnp.int32)
    slots = jnp.zeros((32, 128), jnp.int32)
    for k in range(8):
        slots = slots + jnp.where(lists[:, k : k + 1] == iota((32, 128), 1), 1 << k, 0)
    for p in range(32):
        asks[p] = slots[p : p + 1, :]
    asked[me] = asks[me]
    rows = turned[1].T
    for k in range(6):
        taps_hot[128 * k : 128 * (k + 1), :] = one_hot(rows[:, k : k + 1].astype(jnp.int32) == iota((128, 384), 1))
    order_taps[...] = ordering(1, z)
    ordered = dot(feats[...], order_taps[...]).astype(BF16)
    own_feats[...] = ordered
    table[0:16] = ordered.reshape(16, 8, 256)
    for copy in copies:
        copy.wait()
    drain(staged.at[1], local_sem.at[2])
    drain(staged_far.at[1], local_sem.at[13])
    held[piece, :, c, 0] = staged[...]
    held[piece_far, 0:2, c, 0] = staged_far[...]
    split_in[piece, c, 0] = staged_in[c, 0]
    split_in[piece_far, c, 0] = staged_in[c, 1]
    with jax.named_scope("w_barrier"):
        pl.semaphore_wait(barrier, 46)

    def far_first(body):
        lax.fori_loop(1, NZ, lambda i, _: (body(NZ - i), 0)[1], 0)

    def ask(slot):
        t = z_of(slot)
        for core in range(2):
            send(asks.at[t * 2 + core], asked.at[me], 0, 0, {"z": t, "c": core})

    def spread(n):
        lo, hi, s0, s1, far = CHUNKS[n]

        def one(slot, _):
            source, p = (staged_far.at[lo:hi], piece_far) if far else (staged.at[lo:hi], piece)
            send(source, held.at[p, lo:hi, c, slot], 5 + n, 7 + n, {"z": z_of(slot)})
            return 0

        lax.fori_loop(max(s0, 1), s1, one, 0)

    def along_z(n):
        return (43, 59) if n == LAST else (5 + n, 7 + n)

    def along_axis(n):
        return (44, 60) if n == LAST else (13 + n, 15 + n)

    def spread_in(n):
        s0, s1, far = SPLIT[n]

        def one(slot, _):
            for h in range(2):
                send(staged_in.at[h, far], split_in.at[core_pieces[h][far], c, slot], *along_z(n), {"z": z_of(slot), "c": h})
            return 0

        if s0 == 0:
            p = (1 - other) * core_pieces[0][far] + other * core_pieces[1][far]
            send(staged_in.at[other, far], split_in.at[p, c, 0], *along_z(n), {"c": other})
        lax.fori_loop(max(s0, 1), s1, one, 0)

    def arrivals(n):
        return split_in.at[0, 0, 0 : 15 if SPLIT[n][0] == 0 else 16]

    far_first(ask)
    send(asks.at[z * 2 + other], asked.at[me], 0, 0, {"c": other})
    for n in range(4):
        spread(n)
    spread_in(4)
    spread_in(5)
    send(cot.at[c], cot.at[c], 1, 1, {"c": other})
    for copy in later:
        copy.wait()
    m32 = iota((32, 1), 0)
    target = jnp.zeros((32, 1), jnp.int32)
    for e in range(8):
        block = choice[0, e // 4, e % 4]
        target = jnp.where((m32 & 7) == e, (block // 2) * 8 + lax.rem(block, 2), target)
    chosen_hot[c] = one_hot(target + 2 * (m32 >> 3) == iota((32, 256), 1))
    order_in[...] = ordering(2, z)
    order_out[...] = ordering(3, z)

    def part(n, p, count, from_slot=None, to_slot=None):
        lo, hi, s0, s1, _ = CHUNKS[n]
        return held.at[pl.ds(p, count), lo:hi, c, s0 if from_slot is None else from_slot : s1 if to_slot is None else to_slot]

    def cross(n, p, count):
        some = part(n, p, count)
        send(some, some, 29 + n, 47 + n, {"c": other})

    def along_a(n):
        lo, hi, s0, s1, far = CHUNKS[n]
        with jax.named_scope(f"w_z{n}"):
            drain(held.at[0, lo:hi, 0, max(s0, 1) : s1], recv_sem.at[7 + n])
        some = part(n, piece_far if far else piece, 1)
        for d in (2, 1, 3):
            send(some, some, 13 + n, 15 + n, a_peer(d)[1])

    def along_b(n):
        lo, hi, s0, s1, far = CHUNKS[n]
        with jax.named_scope(f"w_a{n}"):
            drain(held.at[0:3, lo:hi, 0, s0:s1], recv_sem.at[15 + n])
        if not far:
            for k, d in enumerate((1, 3)):
                send(part(n, b * 4, 4), part(n, b * 4, 4), 21 + n, 23 + 8 * k + n, b_peer(d)[1])
        cross(n, (b_far if far else b) * 4, 4)

    def relay(n):
        lo, hi, s0, s1, _ = CHUNKS[n]
        middle = (s0 + s1) // 2
        for k, d, low, high in ((0, 1, s0, middle), (1, 3, middle, s1)):
            source = lax.rem(b + 4 - d, 4) * 4
            with jax.named_scope(f"w_b{n}"):
                drain(part(n, source, 4), recv_sem.at[23 + 8 * k + n])
            if n in RELAYED:
                send(part(n, source, 4, low, high), part(n, source, 4, low, high), 21 + n, 39 + n, b_peer(d)[1])
            cross(n, source, 4)

    def last(n):
        with jax.named_scope(f"w_f{n}"):
            drain(part(n, b_far * 4, 4), recv_sem.at[39 + n])
        cross(n, b_far * 4, 4)

    def part_in(n, p, count):
        s0, s1, _ = SPLIT[n]
        return split_in.at[pl.ds(p, count), :, s0:s1]

    def split_a(n):
        with jax.named_scope(f"w_z{n}"):
            drain(arrivals(n), recv_sem.at[along_z(n)[1]])
        some = part_in(n, piece_far if SPLIT[n][2] else piece, 1)
        for d in (2, 1, 3):
            send(some, some, *along_axis(n), a_peer(d)[1])

    def split_b(n):
        with jax.named_scope(f"w_a{n}"):
            drain(part_in(n, 0, 3), recv_sem.at[along_axis(n)[1]])
        if not SPLIT[n][2]:
            for k, d in enumerate((1, 3)):
                send(part_in(n, b * 4, 4), part_in(n, b * 4, 4), 21 + n, 23 + 8 * k + n, b_peer(d)[1])

    def split_end(n):
        for k, d in ((0, 1), (1, 3)):
            with jax.named_scope(f"w_b{n}"):
                drain(part_in(n, lax.rem(b + 4 - d, 4) * 4, 4), recv_sem.at[23 + 8 * k + n])

    def crossings(n):
        return 16 if n in RELAYED else 4 if CHUNKS[n][4] else 12

    def crossed(n):
        lo, hi, s0, s1, _ = CHUNKS[n]
        with jax.named_scope(f"w_c{n}"):
            drain(held.at[0 : crossings(n), lo:hi, 0, s0:s1], recv_sem.at[47 + n])

    send(chosen_hot.at[c], chosen_hot.at[c], 4, 4, {"c": other})
    along_a(0)

    with jax.named_scope("w_ask"):
        drain(asked.at[0:31], recv_sem.at[0])
    wants = jnp.broadcast_to(asked[...], (32, 8, 128))
    wants = one_hot(((wants >> iota((32, 8, 128), 1)) & 1) == 1).reshape(256, 128)
    picked_rows = dot(wants, feats[...]).astype(BF16)
    answers[...] = picked_rows.reshape(32, 8, 256)
    table[16 + me] = answers[me]

    def answer(slot):
        t = z_of(slot)
        for core in range(2):
            send(answers.at[t * 2 + core], table.at[16 + me], 2, 2, {"z": t, "c": core})

    far_first(answer)
    send(answers.at[z * 2 + other], table.at[16 + me], 2, 2, {"c": other})
    spread_in(8)
    spread_in(6)

    along_a(1)
    along_b(0)
    along_a(2)
    along_a(3)
    along_b(1)
    relay(0)
    split_a(4)
    split_a(5)
    along_b(2)
    along_b(3)
    relay(1)
    with jax.named_scope("w_rows"):
        drain(table.at[0:31], recv_sem.at[2])
    fetched = table[16:48].reshape(256, 256)
    table[16:48] = dot(fetched, order_taps[...]).astype(BF16).reshape(32, 8, 256)
    for k in range(3):
        got = dot(taps_hot[256 * k : 256 * (k + 1), :], table[...].reshape(384, 256))
        taps[2 * k : 2 * k + 2] = got.astype(BF16).reshape(2, 128, 256)
    split_b(4)
    for n in range(4):
        crossed(n)
    split_b(5)

    def unit(p, u):
        return held[p, u].reshape(256, 128)

    count = counts[0, me]
    alive = jnp.where(iota((128, 128), 0) < count, 1.0, 0.0)
    alive_wide = jnp.concatenate([alive, alive], axis=1)
    for t in range(0, 4, 2):
        total = jnp.zeros((128, 256), F32)
        for k in range(7):
            p, u = (k // 2) * 4 + t, k % 2
            tap = own_feats[...] if k == 0 else taps[k - 1]
            total = total + dot(tap, jnp.concatenate([unit(p, u), unit(p + 1, u)], axis=1))
        hidden[:, 128 * t : 128 * (t + 2)] = total * alive_wide
    h = hidden[...]
    power = jnp.mean(h * h, axis=-1, keepdims=True)
    normed = (h * lax.rsqrt(power + 1e-06) * gain[...]).astype(BF16)

    token = iota((8, 128), 1)
    block_mask = one_hot(((token >> 6) == iota((8, 128), 0)) & (token < count))
    number = jnp.clip(count - 64 * iota((8, 1), 0), 0, 64)
    means = dot(block_mask, normed) / jnp.maximum(number, 1).astype(F32)
    for j in range(4):
        tall[2 * j : 2 * j + 2, :] = means[0:2, 128 * j : 128 * (j + 1)]
    shorts[me] = tall[...].astype(BF16)

    def tell(slot):
        for core in range(2):
            send(shorts.at[me], shorts.at[me], 3, 3, {"z": z_of(slot), "c": core})

    far_first(tell)
    send(shorts.at[me], shorts.at[me], 3, 3, {"c": other})
    spread(7)

    normed_all[c] = dot(normed, order_in[...]).astype(BF16)
    send(normed_all.at[c], normed_all.at[c], 38, 6, {"c": other})
    split_a(6)
    split_a(8)
    split_end(4)
    with jax.named_scope("w_norm"):
        drain(normed_all.at[0], recv_sem.at[6])
    split_end(5)
    split_b(6)
    split_b(8)

    def unit_in(tile, i):
        if tile < 8:
            return split_in[2 * tile + i].reshape(256, 128)
        return held[12 + 2 * c + i, 1].reshape(256, 128)

    def project(rows, tiles):
        upper = jnp.concatenate([unit_in(t, 0) for t in tiles], axis=1)
        lower = jnp.concatenate([unit_in(t, 1) for t in tiles], axis=1)
        return dot(rows[:, :256], upper) + dot(rows[:, 256:], lower)

    tokens = normed_all[...].reshape(256, 512)
    for tiles in ((0, 1), (2, 3), (4, 5), (6, 7), (8,)):
        qkv[:, 128 * tiles[0] : 128 * (tiles[-1] + 1)] = project(tokens, tiles).astype(BF16)

    half = iota((128, 128), 1) < 64
    key = iota((128, 256), 0)
    same_block = (key >> 6) == ((iota((128, 256), 1) & 127) >> 6)
    for core in range(2):
        near_ok = same_block & (key < counts[0, 2 * z + core])
        rows = slice(128 * core, 128 * (core + 1))
        for j in range(3):
            at = 3 * core + j
            q = qkv[rows, 128 * j : 128 * (j + 1)] * jnp.asarray(0.125, BF16)
            none = jnp.zeros_like(q)
            q = jnp.concatenate([jnp.where(half, q, none), jnp.where(half, none, q)], axis=0)
            split_q[at] = q
            near = jnp.where(near_ok, dot_t(qkv[rows, 384 + 128 * j : 384 + 128 * (j + 1)], q), -1e30)
            top = jnp.max(near, axis=0, keepdims=True)
            near = jnp.exp(near - top)
            near_top[at] = top
            near_sum[at] = jnp.sum(near, axis=0, keepdims=True)
            mixed = turned_dot(qkv[rows, 768 + 128 * j : 768 + 128 * (j + 1)], near.astype(BF16))
            near_mix[at, 0:64] = mixed[0:64, 0:128]
            near_mix[at, 64:128] = mixed[64:128, 128:256]
    drain(chosen_hot.at[0], recv_sem.at[4])
    drain(cot.at[0], recv_sem.at[1])

    with jax.named_scope("w_short"):
        drain(shorts.at[0:31], recv_sem.at[3])
    chosen = dot(chosen_hot[...].reshape(64, 256), shorts[...].reshape(256, 128))
    chosen = jnp.concatenate(
        [jnp.concatenate([chosen[32 * k + 8 * j : 32 * k + 8 * j + 8] for j in range(4)], axis=1) for k in range(2)], axis=0
    ).astype(BF16)
    chosen = dot(chosen, order_in[...]).astype(BF16)
    for tiles in ((3, 4), (5, 6), (7, 8)):
        got = project(chosen, tiles)
        for k in range(2):
            picked[k, :, 128 * (tiles[0] - 3) : 128 * (tiles[0] - 1)] = got[8 * k : 8 * k + 8].astype(BF16)
    far_ok = (iota((8, 256), 0) >> 2) == ((iota((8, 256), 1) & 127) >> 6)
    for j in range(3):
        for core in range(2):
            at = 3 * core + j
            alive_row = jnp.where(iota((1, 128), 1) < counts[0, 2 * z + core], 1.0, 0.0)
            far = jnp.where(far_ok, dot_t(picked[core, :, 128 * j : 128 * (j + 1)], split_q[at]), -1e30)
            top = jnp.maximum(near_top[at], jnp.max(far, axis=0, keepdims=True))
            keep, far = jnp.exp(near_top[at] - top), jnp.exp(far - top)
            scale = 1.0 / (near_sum[at] * keep + jnp.sum(far, axis=0, keepdims=True))
            mixed = turned_dot(picked[core, :, 384 + 128 * j : 384 + 128 * (j + 1)], far.astype(BF16))
            for k in range(2):
                rows, cols = slice(64 * k, 64 * (k + 1)), slice(128 * k, 128 * (k + 1))
                both = near_mix[at, rows] * keep[:, cols] + mixed[rows, cols]
                att[core, 128 * j + 64 * k : 128 * j + 64 * (k + 1)] = (both * (scale[:, cols] * alive_row)).astype(BF16)
        if j == 0:
            continue
        g = j - 1
        rows = slice(192 * g, 192 * (g + 1))
        both = jnp.concatenate([att[0, rows], att[1, rows]], axis=1)
        for t in range(0, 4, 2):
            got = dot(both, cot[:, :, 128 * t : 128 * (t + 2)].reshape(256, 256))
            for k in range(2):
                terms[t + k, 4 * g : 4 * g + 4] = got[:, 128 * k : 128 * (k + 1)].astype(BF16).reshape(4, 2, 3, 8, 128)
        for d in (2, 1, 3):
            t, where = a_peer(d)
            send(terms.at[t, 4 * g : 4 * g + 4], across.at[d - 1, 4 * g : 4 * g + 4], 39 + g, 55 + g, where)
    att_all[c] = att[c]
    send(att.at[other], att_all.at[c], 37, 5, {"c": other})
    along_a(7)

    for g in range(2):
        rows = slice(4 * g, 4 * (g + 1))
        with jax.named_scope(f"w_across{g}"):
            drain(across.at[:, rows], recv_sem.at[55 + g])
        total = terms[a, rows].astype(F32)
        for d in range(3):
            total = total + across[d, rows].astype(F32)
        summed[rows] = total.astype(BF16)

        def reduce_z(k, _):
            for core in range(2):

                @pl.when((8 * c + k) * 2 + core != me)
                def _():
                    send(summed.at[k, core], along.at[z], 41, 57, {"z": 8 * c + k, "c": core})

            return 0

        lax.fori_loop(4 * g, 4 * (g + 1), reduce_z, 0)
    along_b(7)
    mine = z // 8 == c

    @pl.when(mine)
    def _():
        along[z] = summed[z - 8 * c, c]

    relay(7)
    with jax.named_scope("w_along"):

        @pl.when(mine)
        def _():
            drain(along.at[0:15], recv_sem.at[57])

        @pl.when(jnp.logical_not(mine))
        def _():
            drain(along, recv_sem.at[57])

    total = along[0].astype(F32)
    for k in range(1, NZ):
        total = total + along[k].astype(F32)
    sender = z // 8
    summed_piece = (1 - sender) * core_pieces[0][0] + sender * core_pieces[1][0]
    final[summed_piece] = total.astype(BF16)

    for dy, dx in sorted(((dy, dx) for dy in range(4) for dx in range(4)), key=lambda d: -(d[0] * (4 - d[0]) + d[1] * (4 - d[1]))):
        if (dy, dx) != (0, 0):
            where = {"y": lax.rem(y + dy, 4), "x": lax.rem(x + dx, 4)}
            send(final.at[summed_piece], final.at[summed_piece], 42, 58, where)
    last(7)
    crossed(7)
    drain(att_all.at[0], recv_sem.at[5])
    attended = turned_dot(att_all[...].reshape(768, 128), order_out[...]).astype(BF16)
    for t in range(0, 4, 2):
        total = hidden[:, 128 * t : 128 * (t + 2)]
        for i in range(3):
            w = jnp.concatenate([unit(4 * i + t, 2), unit(4 * i + t + 1, 2)], axis=1)
            total = total + dot(attended[:, 256 * i : 256 * (i + 1)], w)
        layer[0, :, 128 * t : 128 * (t + 2)] = total.astype(BF16)

    drain(asked.at[0:31], send_sem.at[0])
    drain(cot.at[0], send_sem.at[1])
    drain(table.at[0:31], send_sem.at[2])
    drain(shorts.at[0:31], send_sem.at[3])
    for n, (lo, hi, s0, s1, far) in CHUNKS.items():
        drain(held.at[0, lo:hi, 0, max(s0, 1) : s1], send_sem.at[5 + n])
        drain(held.at[0:3, lo:hi, 0, s0:s1], send_sem.at[13 + n])
        if not far:
            drain(held.at[0 : 12 if n in RELAYED else 8, lo:hi, 0, s0:s1], send_sem.at[21 + n])
        drain(held.at[0 : crossings(n), lo:hi, 0, s0:s1], send_sem.at[29 + n])
    for n, (s0, s1, far) in SPLIT.items():
        drain(arrivals(n), send_sem.at[along_z(n)[0]])
        drain(part_in(n, 0, 3), send_sem.at[along_axis(n)[0]])
        if not far:
            drain(part_in(n, 0, 8), send_sem.at[21 + n])
    drain(chosen_hot.at[0], send_sem.at[4])
    drain(normed_all.at[0], send_sem.at[38])
    drain(att_all.at[0], send_sem.at[37])
    for g in range(2):
        drain(across.at[:, 4 * g : 4 * (g + 1)], send_sem.at[39 + g])

    @pl.when(mine)
    def _():
        drain(along.at[0:15], send_sem.at[41])

    @pl.when(jnp.logical_not(mine))
    def _():
        drain(along, send_sem.at[41])

    with jax.named_scope("w_final"):
        drain(final.at[0:15], recv_sem.at[58])
    factor = (16 * 4096) ** -0.5
    for t in range(4):
        total = final[t].astype(F32)
        for k in range(1, 4):
            total = total + final[4 * k + t].astype(F32)
        grad[:, 128 * t : 128 * (t + 1)] = total.reshape(24, 128) * factor

    drain(final.at[0:15], send_sem.at[42])


def shards(feats, near_map, wanted, counts, choice, conv, gain, inw, outw, cot):
    vmem = pl.BlockSpec(memory_space=pltpu.VMEM)
    hbm = pl.BlockSpec(memory_space=pltpu.HBM)
    v = pltpu.VMEM
    return pl.pallas_call(
        kernel,
        name="layer",
        out_shape=(jax.ShapeDtypeStruct((1, 128, 512), BF16), jax.ShapeDtypeStruct((24, 512), F32)),
        in_specs=[hbm] * 10,
        out_specs=(vmem, vmem),
        scratch_shapes=[
            v((128, 256), BF16),
            v((6, 1, 128), jnp.int32),
            v((1, 1, 8, 32), jnp.int32),
            pltpu.SMEM((1, 32), jnp.int32),
            pltpu.SMEM((1, 2, 4), jnp.int32),
            v((1, 512), F32),
            v((2, 128, 128), F32),
            v((32, 1, 128), jnp.int32),
            v((32, 1, 128), jnp.int32),
            v((48, 8, 256), BF16),
            v((32, 8, 256), BF16),
            v((128, 256), BF16),
            v((768, 384), BF16),
            v((6, 128, 256), BF16),
            v((3, 8, 128), BF16),
            v((2, 8, 128), BF16),
            v((2, 2, 8, 128), BF16),
            v((16, 3, 2, NZ, 8, 128), BF16),
            v((16, 2, NZ, 8, 128), BF16),
            v((128, 512), F32),
            v((2, 128, 512), BF16),
            v((256, 1152), BF16),
            v((8, 128), F32),
            v((32, 8, 128), BF16),
            v((2, 32, 256), BF16),
            v((2, 8, 768), BF16),
            v((6, 256, 128), BF16),
            v((6, 128, 128), F32),
            v((6, 1, 256), F32),
            v((6, 1, 256), F32),
            v((2, 128, 512), BF16),
            v((2, 384, 128), BF16),
            v((2, 384, 128), BF16),
            v((4, 8, 2, 3, 8, 128), BF16),
            v((3, 8, 2, 3, 8, 128), BF16),
            v((8, 2, 3, 8, 128), BF16),
            v((NZ, 3, 8, 128), BF16),
            v((16, 3, 8, 128), BF16),
            v((256, 256), BF16),
            v((512, 512), BF16),
            v((768, 768), BF16),
            pltpu.SemaphoreType.DMA((20,)),
            pltpu.SemaphoreType.DMA((45,)),
            pltpu.SemaphoreType.DMA((61,)),
        ],
        compiler_params=pltpu.CompilerParams(
            collective_id=0, has_side_effects=True, vmem_limit_bytes=VMEM
        ),
    )(
        *(
            pltpu.with_memory_space_constraint(array, pltpu.HBM)
            for array in (
                feats, near_map.transpose(2, 0, 1), wanted.swapaxes(2, 3), counts, choice, conv, gain.reshape(1, -1), inw, outw, cot
            )
        )
    )


def solution(mesh):
    space = ("z", "c")
    dp = ("y", "x")
    torus = Mesh(mesh.devices.reshape(4, 4, 16, 2), dp + space)
    return jax.shard_map(
        shards,
        mesh=torus,
        in_specs=(
            P(dp, space, None),
            P(dp, space, None),
            P(dp, space, None, None),
            P(dp, None),
            P(dp, space, None),
            P(None, space, None),
            P(),
            P(space, None),
            P(space, None),
            P(dp, space, None),
        ),
        out_specs=(P(dp, space, None), P(space, None)),
        check_vma=False,
    )
```
